128 devices in a mesh: seq: 64 (over x, y, z), head: 2 (over core).
Axes of the slice: x: 4, y: 4, z: 4, core: 2. Of those that a mesh axis runs over, the one named last changes fastest.
Arguments:
- tokens: bfloat16 [65536, 2048], P('seq'), may hold values from -6 to 6
- w_query: bfloat16 [2048, 256], P(None, 'head'), may hold values from -0.25 to 0.25
- w_key: bfloat16 [2048, 256], P(None, 'head'), may hold values from -0.25 to 0.25
- w_value: bfloat16 [2048, 2048], P(None, 'head'), may hold values from -0.125 to 0.125
- w_out: bfloat16 [2048, 2048], replicated, may hold values from -1.796875 to 1.796875
Outputs:
- mixed: bfloat16 [65536, 2048], P('seq', 'head')
The draws below stay inside these ranges and needn't reach their ends.
All inputs are finite; a program needn't handle non-finite values.
Results may differ from the reference program's by a relative error of at most 0.011.
Values may be sent and summed in bfloat16 or wider, within the bound.
No kernel may reach another device: no remote copies, remote signals or barrier semaphores. Data moves between devices by JAX's collectives and lax.ppermute only.
A program may use at most 128 MiB of HBM per device.

```python
import jax
import jax.numpy as jnp
from jax import lax

D = 2048
HEADS = 16
KEY_DIM = 16
VALUE_DIM = 128
TOK_DEV = 1024
FEATURES = 273
TOKENS = 65536
N_SEQ = 64


def steps_of(stream_key, extent, split, least, largest):
    factor_of, own = 1.0, jax.random.fold_in(stream_key, 6)
    for axis_at, shards_of in split:
        draws = jnp.exp(jax.random.uniform(jax.random.fold_in(own, axis_at), (shards_of,), jnp.float32, least / len(split), largest / len(split)))
        factor_of = factor_of * jnp.repeat(draws, extent[axis_at] // shards_of).reshape([-1 if axis == axis_at else 1 for axis in range(len(extent))])
    return factor_of


def normal_values(own_key, dims, spread, most, split=(), held_as=jnp.bfloat16):
    result = spread * jax.random.normal(own_key, dims, jnp.float32)
    if split:
        result = result * steps_of(own_key, dims, split, -0.22, 0.18)
    return jnp.clip(result, -most, most).astype(held_as)


def setup_inputs(seed: int = 0) -> dict:
    seeds = jax.random.split(jax.random.key(seed), 6)
    tokens = normal_values(seeds[0], (TOKENS, D), 1.0, 6.0, ((0, 64),))
    w_query = normal_values(seeds[1], (D, HEADS * KEY_DIM), (D // 4) ** -0.5, 0.25, ((1, 2),))
    w_key = normal_values(seeds[2], (D, HEADS * KEY_DIM), (D // 4) ** -0.5, 0.25, ((1, 2),))
    w_value = normal_values(seeds[3], (D, HEADS * VALUE_DIM), D ** -0.5, 0.125, ((1, 2),))
    w_out = normal_values(seeds[4], (HEADS * VALUE_DIM, D), 0.3, 1.796875)
    return dict(tokens=tokens, w_query=w_query, w_key=w_key, w_value=w_value, w_out=w_out)


def taylor_features(rows):
    wide = rows.astype(jnp.float32)
    count = wide.shape[-1]
    outer = (wide[..., :, None] * wide[..., None, :]).reshape(wide.shape[:-1] + (count * count,))
    ones = jnp.ones(wide.shape[:-1] + (1,), jnp.float32)
    joined = jnp.concatenate([ones, wide / (count ** 0.25), outer / ((2.0 * count) ** 0.5)], axis=-1)
    return joined.astype(jnp.bfloat16)


def reference(tokens, w_query, w_key, w_value, w_out):
    def span_step(carry, span_rows):
        prefix, zprefix = carry
        queries = jnp.dot(span_rows, w_query, preferred_element_type=jnp.float32).astype(jnp.bfloat16).reshape(TOK_DEV, HEADS, KEY_DIM)
        key_rows = jnp.dot(span_rows, w_key, preferred_element_type=jnp.float32).astype(jnp.bfloat16).reshape(TOK_DEV, HEADS, KEY_DIM)
        val_rows = jnp.dot(span_rows, w_value, preferred_element_type=jnp.float32).astype(jnp.bfloat16).reshape(TOK_DEV, HEADS, VALUE_DIM)
        query_feat = taylor_features(queries)
        key_feat = taylor_features(key_rows)
        state = jnp.einsum('thf,thv->hfv', key_feat.astype(jnp.float32), val_rows.astype(jnp.float32), precision=lax.Precision.HIGHEST)
        norm_sum = jnp.sum(key_feat.astype(jnp.float32), axis=0)
        prefix_low = prefix.astype(jnp.bfloat16)
        numer_pre = jnp.einsum('thf,hfv->thv', query_feat.astype(jnp.float32), prefix_low.astype(jnp.float32), precision=lax.Precision.HIGHEST)
        denom_pre = jnp.einsum('thf,hf->th', query_feat.astype(jnp.float32), zprefix, precision=lax.Precision.HIGHEST)
        block = min(512, TOK_DEV)
        outputs = []
        for index in range(TOK_DEV // block):
            low = index * block
            high = low + block
            q_block = queries[low:high].astype(jnp.float32)
            k_block = key_rows[:high].astype(jnp.float32)
            scores = jnp.einsum('qhd,khd->hqk', q_block, k_block) / (KEY_DIM ** 0.5)
            taylor = 1.0 + scores + 0.5 * scores * scores
            row_ids = low + jnp.arange(block, dtype=jnp.int32)[:, None]
            col_ids = jnp.arange(high, dtype=jnp.int32)[None, :]
            taylor = jnp.where((col_ids <= row_ids)[None], taylor, 0.0)
            denom = denom_pre[low:high] + jnp.transpose(jnp.sum(taylor, axis=-1))
            taylor_low = taylor.astype(jnp.bfloat16)
            numer_in = jnp.einsum('hqk,khv->qhv', taylor_low.astype(jnp.float32), val_rows[:high].astype(jnp.float32))
            numer = numer_pre[low:high] + numer_in
            outputs.append((numer / denom[..., None]).astype(jnp.bfloat16))
        attended = jnp.concatenate(outputs, axis=0).reshape(TOK_DEV, HEADS * VALUE_DIM)
        mixed_rows = jnp.dot(attended, w_out, preferred_element_type=jnp.float32).astype(jnp.bfloat16)
        return (prefix + state, zprefix + norm_sum), mixed_rows

    init = (jnp.zeros((HEADS, FEATURES, VALUE_DIM), jnp.float32), jnp.zeros((HEADS, FEATURES), jnp.float32))
    spans = tokens.reshape(N_SEQ, TOK_DEV, D)
    final, mixed = lax.scan(span_step, init, spans)
    return mixed.reshape(TOKENS, D)
```

```python
import jax
import jax.numpy as jnp
import numpy as np
from jax import lax
from jax.sharding import Mesh
from jax.sharding import PartitionSpec as P

KEY_DIM = 16
VALUE_DIM = 128
PACKED = 153
ROWS = 160
SEQ = ("seq_0", "seq_1", "seq_2")
STEPS = (2, 1, 3)


def partner(x, axis, step):
    pairs = [(i, i ^ step) for i in range(4)]
    return lax.ppermute(x, axis, pairs)


def taylor_features(rows):
    wide = rows.astype(jnp.float32)
    count = wide.shape[-1]
    outer = (wide[..., :, None] * wide[..., None, :]).reshape(wide.shape[:-1] + (count * count,))
    ones = jnp.ones(wide.shape[:-1] + (1,), jnp.float32)
    joined = jnp.concatenate([ones, wide / count**0.25, outer / (2.0 * count) ** 0.5], axis=-1)
    return joined.astype(jnp.bfloat16)


def packing_tables(count):
    kept_rows = list(range(1 + count))
    mirror_rows = list(range(1 + count))
    off_diagonal = [False] * (1 + count)
    for first in range(count):
        for second in range(first, count):
            kept_rows.append(1 + count + first * count + second)
            mirror_rows.append(1 + count + second * count + first)
            off_diagonal.append(first != second)
    return (np.array(kept_rows, np.int32), np.array(mirror_rows, np.int32), np.array(off_diagonal))


def exclusive_prefix(state):
    at_z, at_y, at_x = (lax.axis_index(SEQ[2]), lax.axis_index(SEQ[1]), lax.axis_index(SEQ[0]))
    quarters = state.reshape(4, 2, *state.shape[1:])

    def quarter(index):
        return lax.dynamic_index_in_dim(quarters, index, 0, False)

    f32 = jnp.float32
    parts = {0: quarter(at_z)}
    for step in STEPS:
        parts[step] = partner(quarter(at_z ^ step), SEQ[2], step)
    parts = {step: part.astype(f32) for step, part in parts.items()}
    total = sum(parts.values())
    base = jnp.zeros_like(total)
    for axis, at in ((SEQ[1], at_y), (SEQ[0], at_x)):
        low = total.astype(jnp.bfloat16)
        for step in STEPS:
            got = partner(low, axis, step).astype(f32)
            base = base + jnp.where((at ^ step) < at, got, 0.0)
            total = total + got

    def prefix_at(step):
        out = base
        for other, part in parts.items():
            out = out + jnp.where((at_z ^ other) < (at_z ^ step), part, 0.0)
        return out.astype(jnp.bfloat16)

    back = {0: prefix_at(0)}
    for step in STEPS:
        back[step] = partner(prefix_at(step), SEQ[2], step)
    stacked = jnp.stack([back[step] for step in range(4)])
    pieces = [lax.dynamic_index_in_dim(stacked, at_z ^ q, 0, False) for q in range(4)]
    return jnp.concatenate(pieces, axis=0)


def per_device(tokens, w_query, w_key, w_value, w_out):
    tok_rows = tokens.shape[0]
    heads_here = w_query.shape[1] // KEY_DIM
    key_rows = (
        jnp.dot(tokens, w_key, preferred_element_type=jnp.float32)
        .astype(jnp.bfloat16)
        .reshape(tok_rows, heads_here, KEY_DIM)
    )
    val_rows = (
        jnp.dot(tokens, w_value, preferred_element_type=jnp.float32)
        .astype(jnp.bfloat16)
        .reshape(tok_rows, heads_here, VALUE_DIM)
    )
    key_feat = taylor_features(key_rows)
    state = jnp.einsum("thf,thv->hfv", key_feat, val_rows, preferred_element_type=jnp.float32)
    norm_sum = jnp.sum(key_feat.astype(jnp.float32), axis=0)
    kept_rows, mirror_rows, off_diagonal = packing_tables(KEY_DIM)
    packed_state = state[:, kept_rows] + jnp.where(
        off_diagonal[None, :, None], state[:, mirror_rows], 0.0
    )
    packed_norm = norm_sum[:, kept_rows] + jnp.where(
        off_diagonal[None, :], norm_sum[:, mirror_rows], 0.0
    )
    norm_lanes = jnp.pad(packed_norm, ((0, 0), (0, 256 - PACKED))).reshape(heads_here, 2, 128)
    joined = jnp.concatenate(
        [packed_state, norm_lanes, jnp.zeros((heads_here, ROWS - PACKED - 2, 128), jnp.float32)], 1
    ).astype(jnp.bfloat16)
    queries = (
        jnp.dot(tokens, w_query, preferred_element_type=jnp.float32)
        .astype(jnp.bfloat16)
        .reshape(tok_rows, heads_here, KEY_DIM)
    )
    query_feat = taylor_features(queries)
    prefix = exclusive_prefix(joined)
    used_feat = query_feat[:, :, kept_rows]
    prefix_low = prefix[:, :PACKED]
    zprefix = prefix[:, PACKED : PACKED + 2].reshape(heads_here, 256)[:, :PACKED]
    numer_pre = jnp.einsum(
        "thf,hfv->thv", used_feat, prefix_low, preferred_element_type=jnp.float32
    )
    denom_pre = jnp.einsum("thf,hf->th", used_feat, zprefix, preferred_element_type=jnp.float32)
    block = min(512, tok_rows)
    outputs = []
    for index in range(tok_rows // block):
        low = index * block
        high = low + block
        scores = (
            jnp.einsum(
                "qhd,khd->hqk",
                queries[low:high],
                key_rows[:high],
                preferred_element_type=jnp.float32,
            )
            / KEY_DIM**0.5
        )
        taylor = 1.0 + scores + 0.5 * scores * scores
        row_ids = low + jnp.arange(block, dtype=jnp.int32)[:, None]
        col_ids = jnp.arange(high, dtype=jnp.int32)[None, :]
        taylor = jnp.where((col_ids <= row_ids)[None], taylor, 0.0)
        denom = denom_pre[low:high] + jnp.transpose(jnp.sum(taylor, axis=-1))
        numer_in = jnp.einsum(
            "hqk,khv->qhv",
            taylor.astype(jnp.bfloat16),
            val_rows[:high],
            preferred_element_type=jnp.float32,
        )
        numer = numer_pre[low:high] + numer_in
        outputs.append((numer / denom[..., None]).astype(jnp.bfloat16))
    attended = jnp.concatenate(outputs, axis=0).reshape(tok_rows, heads_here * VALUE_DIM)
    other = lax.ppermute(attended, "head", [(0, 1), (1, 0)])
    own = lax.axis_index("head")
    width = heads_here * VALUE_DIM
    own_block = lax.dynamic_slice(w_out, (own * width, own * width), (width, width))
    other_block = lax.dynamic_slice(w_out, ((1 - own) * width, own * width), (width, width))
    mixed = jnp.dot(attended, own_block, preferred_element_type=jnp.float32)
    mixed = mixed + jnp.dot(other, other_block, preferred_element_type=jnp.float32)
    return mixed.astype(jnp.bfloat16)


def solution(mesh):
    split = Mesh(
        mesh.devices.reshape(4, 4, 4, mesh.shape["head"]), ("seq_0", "seq_1", "seq_2", "head")
    )
    in_specs = (P(SEQ, None), P(None, "head"), P(None, "head"), P(None, "head"), P())
    out_specs = P(SEQ, "head")
    return jax.shard_map(
        per_device, mesh=split, in_specs=in_specs, out_specs=out_specs, check_vma=False
    )
```

```python
import functools

import jax
import jax.numpy as jnp
import numpy as np
from jax import lax
from jax.experimental import pallas as pl
from jax.experimental.pallas import tpu as pltpu
from jax.sharding import Mesh
from jax.sharding import PartitionSpec as P

KEY_DIM = 16
VALUE_DIM = 128
PACKED = 153
ROWS = 160
CHUNK = 256
SEQ = ("seq_0", "seq_1", "seq_2")
STEPS = (2, 1, 3)
SLOTS = (0, 2, 1, 3)
F32, BF16 = (jnp.float32, jnp.bfloat16)
VMEM = pl.BlockSpec(memory_space=pltpu.VMEM)
SMEM = pl.BlockSpec(memory_space=pltpu.SMEM)
ANY = pl.BlockSpec(memory_space=pl.ANY)
NN = (((1,), (0,)), ((), ()))


def mm(a, b):
    return lax.dot_general(a, b, NN, preferred_element_type=F32)


def feature_tables():
    first, second, scale = ([-1] * ROWS, [-1] * ROWS, [0.0] * ROWS)
    for d in range(9):
        for a in range(16 if d < 8 else 8):
            row = 16 * d + a
            first[row], second[row] = (a, (a + d) % 16)
            scale[row] = 1.0 / 32.0 if d == 0 else 1.0 / 16.0
    for a in range(16):
        first[136 + a], scale[136 + a] = (a, 0.25)
    scale[152] = 1.0
    table = np.zeros((8, ROWS), np.float32)
    table[0], table[1], table[2] = (first, second, scale)
    table[3, 152] = 1.0
    table[4, 136:153] = scale[136:153]
    return table


def key_features(u):
    tok = u.shape[1]
    blocks = [u * u]
    for d in range(1, 9):
        blocks.append(u * pltpu.roll(u, 16 - d, 0))
    blocks[8] = blocks[8][:8]
    row = lax.broadcasted_iota(jnp.int32, (8, tok), 0)
    tail = jnp.where(row == 0, 1.0, 0.0)
    return jnp.concatenate(blocks + [u, tail], axis=0).astype(BF16)


def norm_rows(norm):
    top = jnp.transpose(norm[:128])[:1]
    rest = jnp.concatenate([norm[128:], jnp.zeros((96, 128), F32)], axis=0)
    low = jnp.transpose(rest)[:1]
    row = lax.broadcasted_iota(jnp.int32, (8, 128), 0)
    return jnp.where(row == 1, top, jnp.where(row == 2, low, 0.0))


def head_kernel(
    order, x_hbm, wk_hbm, wq_hbm, wv_hbm,
    q_out, kt_out, val_out, local_out, s0, s1, s2, s3,
    x, wkq, wv, acc, kt, x_sem, w_sem, v_sem,
):
    tok, width = x.shape
    cuts = 4
    cut = width // cuts
    kd = wk_hbm.shape[1]

    def wcopy(j, src, half):
        rows = pl.ds(j * cut, cut)
        return pltpu.make_async_copy(
            src.at[rows], wkq.at[rows, pl.ds(half * kd, kd)], w_sem.at[2 * j + half]
        )

    def xcopy(j):
        cols = pl.ds(j * cut, cut)
        return pltpu.make_async_copy(x_hbm.at[:, cols], x.at[:, cols], x_sem.at[j])

    def vcopy(s):
        start = pl.multiple_of(order[s] * 256, 256)
        return pltpu.make_async_copy(wv_hbm.at[:, pl.ds(start, 256)], wv.at[s], v_sem.at[s])

    for j in range(cuts):
        wcopy(j, wk_hbm, 0).start()
        wcopy(j, wq_hbm, 1).start()
        xcopy(j).start()
    for s in range(4):
        vcopy(s).start()
    for j in range(cuts):
        wcopy(j, wk_hbm, 0).wait()
        wcopy(j, wq_hbm, 1).wait()
        xcopy(j).wait()
        part = mm(x[:, j * cut : (j + 1) * cut], wkq[j * cut : (j + 1) * cut])
        acc[...] = part if j == 0 else acc[...] + part
    q_out[...] = acc[:, kd:].astype(BF16)
    keys = jnp.transpose(acc[:, :kd].astype(BF16).astype(F32))
    kt[...] = keys
    kt_out[...] = keys.astype(BF16)
    ones = jnp.ones((CHUNK, 128), BF16)
    for s, state in enumerate((s0, s1, s2, s3)):
        vcopy(s).wait()
        val = mm(x[...], wv[s]).astype(BF16)
        val_out[s] = val
        for h in range(2):
            at = pl.multiple_of((order[s] * 2 + h) * 16, 16)
            feat = key_features(kt[pl.ds(at, 16), :])
            run = None
            for c in range(tok // CHUNK):
                rows = slice(c * CHUNK, (c + 1) * CHUNK)
                right = jnp.concatenate([val[rows, h * 128 : (h + 1) * 128], ones], axis=1)
                part = mm(feat[:, rows], right)
                run = part if c == 0 else run + part
                if c < tok // CHUNK - 1:
                    local_out[s, h, c] = run.astype(BF16)
            state[h, :152] = run[:152, :128].astype(BF16)
            extra = norm_rows(run[:, 128:])
            row = lax.broadcasted_iota(jnp.int32, (8, 128), 0)
            state[h, 152:] = jnp.where(row == 0, run[152:, :128], extra).astype(BF16)


def head_stage(order, tokens, w_key, w_query, w_value):
    tok, width = tokens.shape
    kd = w_key.shape[1]
    chunks = tok // CHUNK
    shape = jax.ShapeDtypeStruct
    return pl.pallas_call(
        head_kernel,
        out_shape=[
            shape((tok, kd), BF16),
            shape((kd, tok), BF16),
            shape((4, tok, 256), BF16),
            shape((4, 2, chunks - 1, ROWS, 256), BF16),
        ]
        + [shape((2, ROWS, 128), BF16)] * 4,
        in_specs=[SMEM, ANY, ANY, ANY, ANY],
        out_specs=[VMEM] * 8,
        scratch_shapes=[
            pltpu.VMEM((tok, width), BF16),
            pltpu.VMEM((width, 2 * kd), BF16),
            pltpu.VMEM((4, width, 256), BF16),
            pltpu.VMEM((tok, 2 * kd), F32),
            pltpu.VMEM((kd, tok), F32),
            pltpu.SemaphoreType.DMA((4,)),
            pltpu.SemaphoreType.DMA((8,)),
            pltpu.SemaphoreType.DMA((4,)),
        ],
        compiler_params=pltpu.CompilerParams(vmem_limit_bytes=40 * 2**20),
        cost_estimate=pl.CostEstimate(
            flops=6 * 10**9, bytes_accessed=12 * 2**20, transcendentals=0
        ),
        name="head_stage",
    )(order, tokens, w_key, w_query, w_value)


def inner_kernel(slot, order, q_ref, kt_ref, val_ref, local_ref, table_ref, feat_out, part_out):
    tok = q_ref.shape[0]
    ones = jnp.ones((CHUNK, 128), BF16)
    below = lax.broadcasted_iota(jnp.int32, (CHUNK, CHUNK), 0) >= lax.broadcasted_iota(
        jnp.int32, (CHUNK, CHUNK), 1
    )
    first, second, scale = (table_ref[0:1], table_ref[1:2], table_ref[2:3])
    add_first, add_second = (table_ref[3:4], table_ref[4:5])
    entry = lax.broadcasted_iota(jnp.int32, (128, ROWS), 0).astype(F32)
    lane = lax.broadcasted_iota(jnp.int32, (CHUNK, 128), 1)
    for h in range(2):
        at = (order[slot] * 2 + h) * 16
        base = at.astype(F32)
        pick_first = jnp.where((entry == first + base) & (first >= 0), 1.0, 0.0).astype(BF16)
        pick_second = jnp.where((entry == second + base) & (second >= 0), scale, 0.0).astype(BF16)
        mine = (lane >= at) & (lane < at + 16)
        for c in range(tok // CHUNK):
            rows = slice(c * CHUNK, (c + 1) * CHUNK)
            q = q_ref[rows]
            feat = (mm(q, pick_first) + add_first) * (mm(q, pick_second) + add_second)
            feat = feat.astype(BF16)
            feat_out[h, rows] = feat
            own = jnp.where(mine, q.astype(F32) * 0.25, 0.0).astype(BF16)
            s = mm(own, kt_ref[:, rows])
            taylor = jnp.where(below, (0.5 * s + 1.0) * s + 1.0, 0.0).astype(BF16)
            right = jnp.concatenate([val_ref[0, rows, h * 128 : (h + 1) * 128], ones], axis=1)
            part = mm(taylor, right)
            if c > 0:
                part = part + mm(feat, local_ref[0, h, c - 1])
            part_out[h, rows] = part


def inner_stage(slot, order, q, kt, val, local, table):
    tok = q.shape[0]
    shape = jax.ShapeDtypeStruct
    return pl.pallas_call(
        functools.partial(inner_kernel, slot),
        grid=(1,),
        out_shape=[shape((2, tok, ROWS), BF16), shape((2, tok, 256), F32)],
        in_specs=[
            SMEM,
            pl.BlockSpec(q.shape, lambda i: (0, 0)),
            pl.BlockSpec(kt.shape, lambda i: (0, 0)),
            pl.BlockSpec((1,) + val.shape[1:], lambda i: (slot, 0, 0)),
            pl.BlockSpec((1,) + local.shape[1:], lambda i: (slot, 0, 0, 0, 0)),
            pl.BlockSpec(table.shape, lambda i: (0, 0)),
        ],
        out_specs=[
            pl.BlockSpec((2, tok, ROWS), lambda i: (0, 0, 0)),
            pl.BlockSpec((2, tok, 256), lambda i: (0, 0, 0)),
        ],
        compiler_params=pltpu.CompilerParams(vmem_limit_bytes=16 * 2**20),
        cost_estimate=pl.CostEstimate(
            flops=2 * 10**9, bytes_accessed=4 * 2**20, transcendentals=0
        ),
        name="inner_stage",
    )(order, q, kt, val, local, table)


def outer_kernel(count, *refs):
    prefixes, feats, parts, out = (
        refs[:count], refs[count : 2 * count], refs[2 * count : 3 * count], refs[3 * count]
    )
    for i in range(count):
        for h in range(2):
            low = prefixes[i][h]
            wide = low[152:].astype(F32)
            top = jnp.transpose(jnp.broadcast_to(wide[1:2], (128, 128)))
            rest = jnp.transpose(jnp.broadcast_to(wide[2:3], (128, 128)))[:32]
            norm = jnp.concatenate([top, rest], axis=0).astype(BF16)
            right = jnp.concatenate([low, norm], axis=1)
            both = mm(feats[i][h], right) + parts[i][h]
            cols = slice(i * 256 + h * 128, i * 256 + (h + 1) * 128)
            out[:, cols] = (both[:, :128] / both[:, 128:]).astype(BF16)


def outer_stage(prefixes, feats, parts):
    count = len(prefixes)
    tok = feats[0].shape[1]
    return pl.pallas_call(
        functools.partial(outer_kernel, count),
        out_shape=jax.ShapeDtypeStruct((tok, 256 * count), BF16),
        in_specs=[VMEM] * (3 * count),
        out_specs=VMEM,
        compiler_params=pltpu.CompilerParams(vmem_limit_bytes=24 * 2**20),
        cost_estimate=pl.CostEstimate(
            flops=3 * 10**8 * count, bytes_accessed=2**20 * count, transcendentals=0
        ),
        name="outer_stage",
    )(*prefixes, *feats, *parts)


def out_kernel(base, first, order, own, a_ref, w_hbm, *rest):
    if first:
        out, w, sem = rest
    else:
        acc, out, w, sem = rest
    cols = pl.ds(pl.multiple_of(own[0] * 1024, 1024), 1024)

    def copy(s):
        start = pl.multiple_of(own[base] * 1024 + order[s] * 256, 256)
        return pltpu.make_async_copy(
            w_hbm.at[pl.ds(start, 256), cols], w.at[pl.ds(s * 256, 256)], sem.at[s]
        )

    for s in range(4):
        copy(s).start()
    for s in range(4):
        copy(s).wait()
    for c in range(a_ref.shape[0] // CHUNK):
        rows = slice(c * CHUNK, (c + 1) * CHUNK)
        part = mm(a_ref[rows], w[...])
        out[rows] = part if first else (part + acc[rows]).astype(BF16)


def out_stage(base, order, own, attended, w_out, acc=None):
    first = acc is None
    tok = attended.shape[0]
    return pl.pallas_call(
        functools.partial(out_kernel, base, first),
        out_shape=jax.ShapeDtypeStruct((tok, 1024), F32 if first else BF16),
        in_specs=[SMEM, SMEM, VMEM, ANY] + ([] if first else [VMEM]),
        out_specs=VMEM,
        scratch_shapes=[pltpu.VMEM((1024, 1024), BF16), pltpu.SemaphoreType.DMA((4,))],
        compiler_params=pltpu.CompilerParams(vmem_limit_bytes=24 * 2**20),
        cost_estimate=pl.CostEstimate(
            flops=2 * 10**9, bytes_accessed=8 * 2**20, transcendentals=0
        ),
        name="out_stage",
    )(*([order, own, attended, w_out] + ([] if first else [acc])))


def partner(x, axis, step):
    pairs = [(i, i ^ step) for i in range(4)]
    return lax.ppermute(x, axis, pairs)


def exclusive_prefix(states):
    at_z, at_y, at_x = (lax.axis_index(SEQ[2]), lax.axis_index(SEQ[1]), lax.axis_index(SEQ[0]))
    parts = {0: states[0]}
    for step in STEPS:
        parts[step] = partner(states[step], SEQ[2], step)
    parts = {step: part.astype(F32) for step, part in parts.items()}
    total = sum(parts.values())
    base = jnp.zeros_like(total)
    for axis, at in ((SEQ[1], at_y), (SEQ[0], at_x)):
        low = total.astype(BF16)
        for step in STEPS:
            got = partner(low, axis, step).astype(F32)
            base = base + jnp.where((at ^ step) < at, got, 0.0)
            total = total + got

    def prefix_at(step):
        out = base
        for other, part in parts.items():
            out = out + jnp.where((at_z ^ other) < (at_z ^ step), part, 0.0)
        return out.astype(BF16)

    back = {0: prefix_at(0)}
    for step in STEPS:
        back[step] = partner(prefix_at(step), SEQ[2], step)
    return back


def per_device(tokens, w_query, w_key, w_value, w_out):
    order = lax.axis_index(SEQ[2]) ^ jnp.array(SLOTS, jnp.int32)
    own = lax.axis_index("head") ^ jnp.array([0, 1], jnp.int32)
    table = jnp.asarray(feature_tables())
    q, kt, val, local, *states = head_stage(order, tokens, w_key, w_query, w_value)
    back = exclusive_prefix(dict(zip(SLOTS, states)))
    inner = [inner_stage(s, order, q, kt, val, local, table) for s in range(4)]
    feats, parts = ([pair[0] for pair in inner], [pair[1] for pair in inner])
    prefixes = [back[step] for step in SLOTS]
    attended = outer_stage(prefixes, feats, parts)
    other = lax.ppermute(attended, "head", [(0, 1), (1, 0)])
    acc = out_stage(0, order, own, attended, w_out)
    return out_stage(1, order, own, other, w_out, acc)


def solution(mesh):
    split = Mesh(
        mesh.devices.reshape(4, 4, 4, mesh.shape["head"]), ("seq_0", "seq_1", "seq_2", "head")
    )
    in_specs = (P(SEQ, None), P(None, "head"), P(None, "head"), P(None, "head"), P())
    out_specs = P(SEQ, "head")
    return jax.shard_map(
        per_device, mesh=split, in_specs=in_specs, out_specs=out_specs, check_vma=False
    )
```

```python
import functools

import jax
import jax.numpy as jnp
import numpy as np
from jax import lax
from jax.experimental import pallas as pl
from jax.experimental.pallas import tpu as pltpu
from jax.sharding import Mesh
from jax.sharding import PartitionSpec as P

KEY_DIM = 16
VALUE_DIM = 128
PACKED = 153
ROWS = 160
CHUNK = 256
SEQ = ("seq_0", "seq_1", "seq_2")
STEPS = (2, 1, 3)
MIB = 2**20
HEAD_LIMIT, FETCH_LIMIT, OUT_LIMIT = (48 * MIB, 44 * MIB, 20 * MIB)
SLOTS = (0, 2, 1, 3)
F32, BF16 = (jnp.float32, jnp.bfloat16)
VMEM = pl.BlockSpec(memory_space=pltpu.VMEM)
SMEM = pl.BlockSpec(memory_space=pltpu.SMEM)
ANY = pl.BlockSpec(memory_space=pl.ANY)
NN = (((1,), (0,)), ((), ()))


def mm(a, b):
    return lax.dot_general(a, b, NN, preferred_element_type=F32)


def quarter_of(step):
    return lax.axis_index(SEQ[2]) ^ step


def feature_tables():
    first, second, scale = ([-1] * ROWS, [-1] * ROWS, [0.0] * ROWS)
    for d in range(9):
        for a in range(16 if d < 8 else 8):
            row = 16 * d + a
            first[row], second[row] = (a, (a + d) % 16)
            scale[row] = 1.0 / 32.0 if d == 0 else 1.0 / 16.0
    for a in range(16):
        first[136 + a], scale[136 + a] = (a, 0.25)
    scale[152] = 1.0
    table = np.zeros((8, ROWS), np.float32)
    table[0], table[1], table[2] = (first, second, scale)
    table[3, 152] = 1.0
    table[4, 136:153] = scale[136:153]
    return table


def key_features(u):
    tok = u.shape[1]
    blocks = [u * u]
    for d in range(1, 9):
        blocks.append(u * pltpu.roll(u, 16 - d, 0))
    blocks[8] = blocks[8][:8]
    row = lax.broadcasted_iota(jnp.int32, (8, tok), 0)
    tail = jnp.where(row == 0, 1.0, 0.0)
    return jnp.concatenate(blocks + [u, tail], axis=0).astype(BF16)


def norm_rows(norm):
    top = jnp.transpose(norm[:128])[:1]
    rest = jnp.concatenate([norm[128:], jnp.zeros((96, 128), F32)], axis=0)
    low = jnp.transpose(rest)[:1]
    row = lax.broadcasted_iota(jnp.int32, (8, 128), 0)
    return jnp.where(row == 1, top, jnp.where(row == 2, low, 0.0))


def head_kernel(
    x_hbm, wk_hbm, wq_hbm, wv_hbm,
    q_out, kt_out, val_out, local_out, s0, s1, s2, s3,
    x, wkq, wv, acc, kt, x_sem, w_sem, v_sem,
):
    tok, width = x.shape
    cuts = 4
    cut = width // cuts
    kd = wk_hbm.shape[1]

    def wcopy(j, src, half):
        rows = pl.ds(j * cut, cut)
        return pltpu.make_async_copy(
            src.at[rows], wkq.at[rows, pl.ds(half * kd, kd)], w_sem.at[2 * j + half]
        )

    def xcopy(j):
        cols = pl.ds(j * cut, cut)
        return pltpu.make_async_copy(x_hbm.at[:, cols], x.at[:, cols], x_sem.at[j])

    def vcopy(s):
        start = pl.multiple_of(quarter_of(SLOTS[s]) * 256, 256)
        return pltpu.make_async_copy(wv_hbm.at[:, pl.ds(start, 256)], wv.at[s], v_sem.at[s])

    for j in range(cuts):
        wcopy(j, wk_hbm, 0).start()
        wcopy(j, wq_hbm, 1).start()
        xcopy(j).start()
    for s in range(4):
        vcopy(s).start()
    for j in range(cuts):
        wcopy(j, wk_hbm, 0).wait()
        wcopy(j, wq_hbm, 1).wait()
        xcopy(j).wait()
        part = mm(x[:, j * cut : (j + 1) * cut], wkq[j * cut : (j + 1) * cut])
        acc[...] = part if j == 0 else acc[...] + part
    q_out[...] = acc[:, kd:].astype(BF16)
    keys = jnp.transpose(acc[:, :kd].astype(BF16).astype(F32))
    kt[...] = keys
    kt_out[...] = keys.astype(BF16)
    ones = jnp.ones((CHUNK, 128), BF16)
    for s, state in enumerate((s0, s1, s2, s3)):
        vcopy(s).wait()
        val = mm(x[...], wv[s]).astype(BF16)
        val_out[s] = val
        for h in range(2):
            at = pl.multiple_of((quarter_of(SLOTS[s]) * 2 + h) * 16, 16)
            feat = key_features(kt[pl.ds(at, 16), :])
            run = None
            for c in range(tok // CHUNK):
                rows = slice(c * CHUNK, (c + 1) * CHUNK)
                right = jnp.concatenate([val[rows, h * 128 : (h + 1) * 128], ones], axis=1)
                part = mm(feat[:, rows], right)
                run = part if c == 0 else run + part
                if c < tok // CHUNK - 1:
                    local_out[s, h, c] = run.astype(BF16)
            state[h, :152] = run[:152, :128].astype(BF16)
            extra = norm_rows(run[:, 128:])
            row = lax.broadcasted_iota(jnp.int32, (8, 128), 0)
            state[h, 152:] = jnp.where(row == 0, run[152:, :128], extra).astype(BF16)


def head_stage(tokens, w_key, w_query, w_value):
    tok, width = tokens.shape
    kd = w_key.shape[1]
    chunks = tok // CHUNK
    shape = jax.ShapeDtypeStruct
    return pl.pallas_call(
        head_kernel,
        out_shape=[
            shape((tok, kd), BF16),
            shape((kd, tok), BF16),
            shape((4, tok, 256), BF16),
            shape((4, 2, chunks - 1, ROWS, 256), BF16),
        ]
        + [shape((2, ROWS, 128), BF16)] * 4,
        in_specs=[ANY] * 4,
        out_specs=[VMEM] * 8,
        scratch_shapes=[
            pltpu.VMEM((tok, width), BF16),
            pltpu.VMEM((width, 2 * kd), BF16),
            pltpu.VMEM((4, width, 256), BF16),
            pltpu.VMEM((tok, 2 * kd), F32),
            pltpu.VMEM((kd, tok), F32),
            pltpu.SemaphoreType.DMA((4,)),
            pltpu.SemaphoreType.DMA((8,)),
            pltpu.SemaphoreType.DMA((4,)),
        ],
        compiler_params=pltpu.CompilerParams(vmem_limit_bytes=HEAD_LIMIT),
        cost_estimate=pl.CostEstimate(
            flops=6 * 10**9, bytes_accessed=12 * 2**20, transcendentals=0
        ),
        name="head_stage",
    )(tokens, w_key, w_query, w_value)


def inner_kernel(slot, q_ref, kt_ref, val_ref, local_ref, table_ref, feat_out, part_out):
    tok = q_ref.shape[0]
    ones = jnp.ones((CHUNK, 128), BF16)
    below = lax.broadcasted_iota(jnp.int32, (CHUNK, CHUNK), 0) >= lax.broadcasted_iota(
        jnp.int32, (CHUNK, CHUNK), 1
    )
    first, second, scale = (table_ref[0:1], table_ref[1:2], table_ref[2:3])
    add_first, add_second = (table_ref[3:4], table_ref[4:5])
    entry = lax.broadcasted_iota(jnp.int32, (128, ROWS), 0).astype(F32)
    lane = lax.broadcasted_iota(jnp.int32, (CHUNK, 128), 1)
    for h in range(2):
        at = (quarter_of(SLOTS[slot]) * 2 + h) * 16
        base = at.astype(F32)
        pick_first = jnp.where((entry == first + base) & (first >= 0), 1.0, 0.0).astype(BF16)
        pick_second = jnp.where((entry == second + base) & (second >= 0), scale, 0.0).astype(BF16)
        mine = (lane >= at) & (lane < at + 16)
        for c in range(tok // CHUNK):
            rows = slice(c * CHUNK, (c + 1) * CHUNK)
            q = q_ref[rows]
            feat = (mm(q, pick_first) + add_first) * (mm(q, pick_second) + add_second)
            feat = feat.astype(BF16)
            feat_out[h, rows] = feat
            own = jnp.where(mine, q.astype(F32) * 0.25, 0.0).astype(BF16)
            s = mm(own, kt_ref[:, rows])
            taylor = jnp.where(below, (0.5 * s + 1.0) * s + 1.0, 0.0).astype(BF16)
            right = jnp.concatenate([val_ref[0, rows, h * 128 : (h + 1) * 128], ones], axis=1)
            part = mm(taylor, right)
            if c > 0:
                part = part + mm(feat, local_ref[0, h, c - 1])
            part_out[h, rows] = part


def inner_stage(slot, q, kt, val, local, table):
    tok = q.shape[0]
    shape = jax.ShapeDtypeStruct
    return pl.pallas_call(
        functools.partial(inner_kernel, slot),
        grid=(1,),
        out_shape=[shape((2, tok, ROWS), BF16), shape((2, tok, 256), F32)],
        in_specs=[
            pl.BlockSpec(q.shape, lambda i: (0, 0)),
            pl.BlockSpec(kt.shape, lambda i: (0, 0)),
            pl.BlockSpec((1,) + val.shape[1:], lambda i: (slot, 0, 0)),
            pl.BlockSpec((1,) + local.shape[1:], lambda i: (slot, 0, 0, 0, 0)),
            pl.BlockSpec(table.shape, lambda i: (0, 0)),
        ],
        out_specs=[
            pl.BlockSpec((2, tok, ROWS), lambda i: (0, 0, 0)),
            pl.BlockSpec((2, tok, 256), lambda i: (0, 0, 0)),
        ],
        compiler_params=pltpu.CompilerParams(vmem_limit_bytes=16 * 2**20),
        cost_estimate=pl.CostEstimate(
            flops=2 * 10**9, bytes_accessed=4 * 2**20, transcendentals=0
        ),
        name="inner_stage",
    )(q, kt, val, local, table)


def outer_kernel(count, *refs):
    prefixes, feats, parts, out = (
        refs[:count], refs[count : 2 * count], refs[2 * count : 3 * count], refs[3 * count]
    )
    for i in range(count):
        for h in range(2):
            low = prefixes[i][h]
            wide = low[152:].astype(F32)
            top = jnp.transpose(jnp.broadcast_to(wide[1:2], (128, 128)))
            rest = jnp.transpose(jnp.broadcast_to(wide[2:3], (128, 128)))[:32]
            norm = jnp.concatenate([top, rest], axis=0).astype(BF16)
            right = jnp.concatenate([low, norm], axis=1)
            both = mm(feats[i][h], right) + parts[i][h]
            cols = slice(i * 256 + h * 128, i * 256 + (h + 1) * 128)
            out[:, cols] = (both[:, :128] / both[:, 128:]).astype(BF16)


def outer_stage(prefixes, feats, parts):
    count = len(prefixes)
    tok = feats[0].shape[1]
    return pl.pallas_call(
        functools.partial(outer_kernel, count),
        out_shape=jax.ShapeDtypeStruct((tok, 256 * count), BF16),
        in_specs=[VMEM] * (3 * count),
        out_specs=VMEM,
        compiler_params=pltpu.CompilerParams(vmem_limit_bytes=24 * 2**20),
        cost_estimate=pl.CostEstimate(
            flops=3 * 10**8 * count, bytes_accessed=2**20 * count, transcendentals=0
        ),
        name="outer_stage",
    )(*prefixes, *feats, *parts)


def fetch_kernel(w_hbm, out, sem):
    own = lax.axis_index("head")
    cols = pl.ds(pl.multiple_of(own * 1024, 1024), 1024)

    def copy(half, s):
        start = pl.multiple_of((own ^ half) * 1024 + quarter_of(SLOTS[s]) * 256, 256)
        return pltpu.make_async_copy(
            w_hbm.at[pl.ds(start, 256), cols],
            out.at[half, pl.ds(s * 256, 256)],
            sem.at[half * 4 + s],
        )

    pieces = [copy(half, s) for half in range(2) for s in range(4)]
    for piece in pieces:
        piece.start()
    for piece in pieces:
        piece.wait()


def fetch_stage(w_out):
    return pl.pallas_call(
        fetch_kernel,
        out_shape=jax.ShapeDtypeStruct((2, 1024, 1024), BF16),
        in_specs=[ANY],
        out_specs=VMEM,
        scratch_shapes=[pltpu.SemaphoreType.DMA((8,))],
        compiler_params=pltpu.CompilerParams(vmem_limit_bytes=FETCH_LIMIT),
        cost_estimate=pl.CostEstimate(
            flops=10**9, bytes_accessed=8 * 2**20, transcendentals=0
        ),
        name="fetch_stage",
    )(w_out)


def out_kernel(first, a_ref, w_ref, *rest):
    out = rest[-1]
    for c in range(a_ref.shape[0] // CHUNK):
        rows = slice(c * CHUNK, (c + 1) * CHUNK)
        part = mm(a_ref[rows], w_ref[0])
        out[rows] = part if first else (part + rest[0][rows]).astype(BF16)


def out_stage(half, attended, columns, acc=None):
    first = acc is None
    tok = attended.shape[0]
    whole = pl.BlockSpec((tok, 1024), lambda i: (0, 0))
    return pl.pallas_call(
        functools.partial(out_kernel, first),
        grid=(1,),
        out_shape=jax.ShapeDtypeStruct((tok, 1024), F32 if first else BF16),
        in_specs=[whole, pl.BlockSpec((1, 1024, 1024), lambda i: (half, 0, 0))]
        + ([] if first else [whole]),
        out_specs=whole,
        compiler_params=pltpu.CompilerParams(vmem_limit_bytes=OUT_LIMIT),
        cost_estimate=pl.CostEstimate(
            flops=2 * 10**9, bytes_accessed=8 * 2**20, transcendentals=0
        ),
        name="out_stage",
    )(*([attended, columns] + ([] if first else [acc])))


def partner(x, axis, step):
    pairs = [(i, i ^ step) for i in range(4)]
    return lax.ppermute(x, axis, pairs)


def total_kernel(p0, p1, p2, p3, out):
    total = p0[...].astype(F32) + p1[...].astype(F32)
    out[...] = (total + p2[...].astype(F32) + p3[...].astype(F32)).astype(BF16)


def level_kernel(axis, own, g0, g1, g2, base_in, total, base):
    at = lax.axis_index(axis)
    run, before = (own[...].astype(F32), jnp.zeros(own.shape, F32))
    if base_in is not None:
        before = base_in[...]
    for step, ref in zip(STEPS, (g0, g1, g2)):
        got = ref[...].astype(F32)
        run = run + got
        before = before + got * ((at ^ step) < at).astype(F32)
    if total is not None:
        total[...] = run.astype(BF16)
    base[...] = before


def spread_kernel(own, g0, g1, g2, base_in, p0, p1, p2, p3, o0, o1, o2, o3, base):
    level_kernel(SEQ[0], own, g0, g1, g2, base_in, None, base)
    at = lax.axis_index(SEQ[2])
    parts = [p[...].astype(F32) for p in (p0, p1, p2, p3)]
    for mine, out in zip(SLOTS, (o0, o1, o2, o3)):
        run = base[...]
        for step, part in zip(SLOTS, parts):
            run = run + part * ((at ^ step) < (at ^ mine)).astype(F32)
        out[...] = run.astype(BF16)


def small_call(kernel, outs, name, *args, scratch=(), after=()):
    shape = args[0].shape
    return pl.pallas_call(
        kernel,
        out_shape=[jax.ShapeDtypeStruct(shape, kind) for kind in outs],
        in_specs=[VMEM] * len(args) + [ANY] * len(after),
        out_specs=[VMEM] * len(outs),
        scratch_shapes=list(scratch),
        compiler_params=pltpu.CompilerParams(vmem_limit_bytes=4 * 2**20),
        cost_estimate=pl.CostEstimate(flops=10**6, bytes_accessed=2**20, transcendentals=0),
        name=name,
    )(*args, *after)


def middle_kernel(own, g0, g1, g2, columns, total, base):
    level_kernel(SEQ[1], own, g0, g1, g2, None, total, base)


def exclusive_prefix(states, columns):
    parts = [states[0]] + [
        partner(state, SEQ[2], step) for step, state in zip(STEPS, states[1:])
    ]
    (low,) = small_call(total_kernel, [BF16], "total_stage", *parts)
    got = [partner(low, SEQ[1], step) for step in STEPS]
    total, base = small_call(middle_kernel, [BF16, F32], "middle_stage", low, *got, after=[columns])
    got = [partner(total, SEQ[0], step) for step in STEPS]
    scratch = [pltpu.VMEM(low.shape, F32)]
    outs = small_call(
        spread_kernel, [BF16] * 4, "spread_stage", total, *got, base, *parts, scratch=scratch
    )
    return [outs[0]] + [partner(out, SEQ[2], step) for step, out in zip(STEPS, outs[1:])]


def per_device(tokens, w_query, w_key, w_value, w_out):
    table = jnp.asarray(feature_tables())
    q, kt, val, local, *states = head_stage(tokens, w_key, w_query, w_value)
    columns = fetch_stage(w_out)
    prefixes = exclusive_prefix(states, columns)
    inner = [inner_stage(s, q, kt, val, local, table) for s in range(4)]
    feats, parts = ([pair[0] for pair in inner], [pair[1] for pair in inner])
    attended = outer_stage(prefixes, feats, parts)
    other = lax.ppermute(attended, "head", [(0, 1), (1, 0)])
    acc = out_stage(0, attended, columns)
    return out_stage(1, other, columns, acc)


def solution(mesh):
    split = Mesh(
        mesh.devices.reshape(4, 4, 4, mesh.shape["head"]), ("seq_0", "seq_1", "seq_2", "head")
    )
    in_specs = (P(SEQ, None), P(None, "head"), P(None, "head"), P(None, "head"), P())
    out_specs = P(SEQ, "head")
    return jax.shard_map(
        per_device, mesh=split, in_specs=in_specs, out_specs=out_specs, check_vma=False
    )
```

```python
import functools

import jax
import jax.numpy as jnp
import numpy as np
from jax import lax
from jax.experimental import pallas as pl
from jax.experimental.pallas import tpu as pltpu
from jax.sharding import Mesh
from jax.sharding import PartitionSpec as P


ROWS = 160
CHUNK = 256
SEQ = ("seq_0", "seq_1", "seq_2")
STEPS = (2, 1, 3)
MIB = 2**20
HEAD_LIMIT, FETCH_LIMIT, OUT_LIMIT = (48 * MIB, 44 * MIB, 20 * MIB)
SLOTS = (0, 2, 1, 3)
OUT_STEPS = (0, 1, 3, 2)
F32, BF16 = (jnp.float32, jnp.bfloat16)
VMEM = pl.BlockSpec(memory_space=pltpu.VMEM)
SMEM = pl.BlockSpec(memory_space=pltpu.SMEM)
ANY = pl.BlockSpec(memory_space=pl.ANY)
NN = (((1,), (0,)), ((), ()))


def mm(a, b):
    return lax.dot_general(a, b, NN, preferred_element_type=F32)


def quarter_of(step):
    return lax.axis_index(SEQ[2]) ^ step


def feature_tables():
    first, second, scale = ([-1] * ROWS, [-1] * ROWS, [0.0] * ROWS)
    for d in range(9):
        for a in range(16 if d < 8 else 8):
            row = 16 * d + a
            first[row], second[row] = (a, (a + d) % 16)
            scale[row] = 1.0 / 32.0 if d == 0 else 1.0 / 16.0
    for a in range(16):
        first[136 + a], scale[136 + a] = (a, 0.25)
    scale[152] = 1.0
    table = np.zeros((8, ROWS), np.float32)
    table[0], table[1], table[2] = (first, second, scale)
    table[3, 152] = 1.0
    table[4, 136:153] = scale[136:153]
    return table


def key_features(u):
    tok = u.shape[1]
    blocks = [u * u]
    for d in range(1, 9):
        blocks.append(u * pltpu.roll(u, 16 - d, 0))
    blocks[8] = blocks[8][:8]
    row = lax.broadcasted_iota(jnp.int32, (8, tok), 0)
    tail = jnp.where(row == 0, 1.0, 0.0)
    return jnp.concatenate(blocks + [u, tail], axis=0).astype(BF16)


def norm_rows(norm):
    top = jnp.transpose(norm[:128])[:1]
    rest = jnp.concatenate([norm[128:], jnp.zeros((96, 128), F32)], axis=0)
    low = jnp.transpose(rest)[:1]
    row = lax.broadcasted_iota(jnp.int32, (8, 128), 0)
    return jnp.where(row == 1, top, jnp.where(row == 2, low, 0.0))


def head_kernel(
    x_hbm, wk_hbm, wq_hbm, wv_hbm,
    q_out, kt_out, val_out, local_out, s0, s1, s2, s3,
    x, wkq, wv, acc, kt, x_sem, w_sem, v_sem,
):
    tok, width = x.shape
    cuts = 4
    cut = width // cuts
    kd = wk_hbm.shape[1]

    def wcopy(j, src, half):
        rows = pl.ds(j * cut, cut)
        return pltpu.make_async_copy(
            src.at[rows], wkq.at[rows, pl.ds(half * kd, kd)], w_sem.at[2 * j + half]
        )

    def xcopy(j):
        cols = pl.ds(j * cut, cut)
        return pltpu.make_async_copy(x_hbm.at[:, cols], x.at[:, cols], x_sem.at[j])

    def vcopy(s):
        start = pl.multiple_of(quarter_of(SLOTS[s]) * 256, 256)
        return pltpu.make_async_copy(
            wv_hbm.at[:, pl.ds(start, 256)],
            wv.at[s // 2, :, pl.ds(s % 2 * 256, 256)],
            v_sem.at[s],
        )

    for j in range(cuts):
        wcopy(j, wk_hbm, 0).start()
        wcopy(j, wq_hbm, 1).start()
        xcopy(j).start()
    for s in range(4):
        vcopy(s).start()
    for j in range(cuts):
        wcopy(j, wk_hbm, 0).wait()
        wcopy(j, wq_hbm, 1).wait()
        xcopy(j).wait()
        cols = slice(j * cut, (j + 1) * cut)
        for rows in (slice(0, tok // 2), slice(tok // 2, tok)):
            part = mm(x[rows, cols], wkq[cols])
            acc[rows] = part if j == 0 else acc[rows] + part
    q_out[...] = acc[:, kd:].astype(BF16)
    keys = jnp.transpose(acc[:, :kd].astype(BF16).astype(F32))
    kt[...] = keys
    kt_out[...] = keys.astype(BF16)
    ones = jnp.ones((CHUNK, 128), BF16)
    for s, state in enumerate((s0, s1, s2, s3)):
        if s % 2 == 0:
            vcopy(s).wait()
            vcopy(s + 1).wait()
            pair = mm(x[...], wv[s // 2]).astype(BF16)
        val = pair[:, s % 2 * 256 : s % 2 * 256 + 256]
        val_out[s] = val
        for h in range(2):
            at = pl.multiple_of((quarter_of(SLOTS[s]) * 2 + h) * 16, 16)
            feat = key_features(kt[pl.ds(at, 16), :])
            run = None
            for c in range(tok // CHUNK):
                rows = slice(c * CHUNK, (c + 1) * CHUNK)
                right = jnp.concatenate([val[rows, h * 128 : (h + 1) * 128], ones], axis=1)
                part = mm(feat[:, rows], right)
                run = part if c == 0 else run + part
                if c < tok // CHUNK - 1:
                    local_out[s, h, c] = run.astype(BF16)
            state[h, :152] = run[:152, :128].astype(BF16)
            extra = norm_rows(run[:, 128:])
            row = lax.broadcasted_iota(jnp.int32, (8, 128), 0)
            state[h, 152:] = jnp.where(row == 0, run[152:, :128], extra).astype(BF16)


def head_stage(tokens, w_key, w_query, w_value):
    tok, width = tokens.shape
    kd = w_key.shape[1]
    chunks = tok // CHUNK
    shape = jax.ShapeDtypeStruct
    return pl.pallas_call(
        head_kernel,
        out_shape=[
            shape((tok, kd), BF16),
            shape((kd, tok), BF16),
            shape((4, tok, 256), BF16),
            shape((4, 2, chunks - 1, ROWS, 256), BF16),
        ]
        + [shape((2, ROWS, 128), BF16)] * 4,
        in_specs=[ANY] * 4,
        out_specs=[VMEM] * 8,
        scratch_shapes=[
            pltpu.VMEM((tok, width), BF16),
            pltpu.VMEM((width, 2 * kd), BF16),
            pltpu.VMEM((2, width, 512), BF16),
            pltpu.VMEM((tok, 2 * kd), F32),
            pltpu.VMEM((kd, tok), F32),
            pltpu.SemaphoreType.DMA((4,)),
            pltpu.SemaphoreType.DMA((8,)),
            pltpu.SemaphoreType.DMA((4,)),
        ],
        compiler_params=pltpu.CompilerParams(vmem_limit_bytes=HEAD_LIMIT),
        cost_estimate=pl.CostEstimate(
            flops=6 * 10**9, bytes_accessed=12 * 2**20, transcendentals=0
        ),
        name="head_stage",
    )(tokens, w_key, w_query, w_value)


def inner_kernel(slot, q_ref, kt_ref, val_ref, local_ref, table_ref, feat_out, part_out):
    tok = q_ref.shape[0]
    ones = jnp.ones((CHUNK, 128), BF16)
    below = lax.broadcasted_iota(jnp.int32, (CHUNK, CHUNK), 0) >= lax.broadcasted_iota(
        jnp.int32, (CHUNK, CHUNK), 1
    )
    first, second, scale = (table_ref[0:1], table_ref[1:2], table_ref[2:3])
    add_first, add_second = (table_ref[3:4], table_ref[4:5])
    entry = lax.broadcasted_iota(jnp.int32, (128, ROWS), 0).astype(F32)
    lane = lax.broadcasted_iota(jnp.int32, (CHUNK, 128), 1)
    for h in range(2):
        at = (quarter_of(SLOTS[slot]) * 2 + h) * 16
        base = at.astype(F32)
        pick_first = jnp.where((entry == first + base) & (first >= 0), 1.0, 0.0).astype(BF16)
        pick_second = jnp.where((entry == second + base) & (second >= 0), scale, 0.0).astype(BF16)
        mine = (lane >= at) & (lane < at + 16)
        for c in range(tok // CHUNK):
            rows = slice(c * CHUNK, (c + 1) * CHUNK)
            q = q_ref[rows]
            feat = (mm(q, pick_first) + add_first) * (mm(q, pick_second) + add_second)
            feat = feat.astype(BF16)
            feat_out[h, rows] = feat
            own = jnp.where(mine, q.astype(F32) * 0.25, 0.0).astype(BF16)
            s = mm(own, kt_ref[:, rows])
            taylor = jnp.where(below, (0.5 * s + 1.0) * s + 1.0, 0.0).astype(BF16)
            right = jnp.concatenate([val_ref[0, rows, h * 128 : (h + 1) * 128], ones], axis=1)
            part = mm(taylor, right)
            if c > 0:
                part = part + mm(feat, local_ref[0, h, c - 1])
            part_out[h, rows] = part


def inner_stage(slot, q, kt, val, local, table):
    tok = q.shape[0]
    shape = jax.ShapeDtypeStruct
    return pl.pallas_call(
        functools.partial(inner_kernel, slot),
        grid=(1,),
        out_shape=[shape((2, tok, ROWS), BF16), shape((2, tok, 256), F32)],
        in_specs=[
            pl.BlockSpec(q.shape, lambda i: (0, 0)),
            pl.BlockSpec(kt.shape, lambda i: (0, 0)),
            pl.BlockSpec((1,) + val.shape[1:], lambda i: (slot, 0, 0)),
            pl.BlockSpec((1,) + local.shape[1:], lambda i: (slot, 0, 0, 0, 0)),
            pl.BlockSpec(table.shape, lambda i: (0, 0)),
        ],
        out_specs=[
            pl.BlockSpec((2, tok, ROWS), lambda i: (0, 0, 0)),
            pl.BlockSpec((2, tok, 256), lambda i: (0, 0, 0)),
        ],
        compiler_params=pltpu.CompilerParams(vmem_limit_bytes=16 * 2**20),
        cost_estimate=pl.CostEstimate(
            flops=2 * 10**9, bytes_accessed=4 * 2**20, transcendentals=0
        ),
        name="inner_stage",
    )(q, kt, val, local, table)


def outer_kernel(count, *refs):
    prefixes, feats, parts, out = (
        refs[:count], refs[count : 2 * count], refs[2 * count : 3 * count], refs[3 * count]
    )
    for i in range(count):
        for h in range(2):
            low = prefixes[i][h]
            wide = low[152:].astype(F32)
            top = jnp.transpose(jnp.broadcast_to(wide[1:2], (128, 128)))
            rest = jnp.transpose(jnp.broadcast_to(wide[2:3], (128, 128)))[:32]
            norm = jnp.concatenate([top, rest], axis=0).astype(BF16)
            right = jnp.concatenate([low, norm], axis=1)
            both = mm(feats[i][h], right) + parts[i][h]
            cols = slice(i * 256 + h * 128, i * 256 + (h + 1) * 128)
            out[:, cols] = (both[:, :128] / both[:, 128:]).astype(BF16)


def outer_stage(prefixes, feats, parts):
    count = len(prefixes)
    tok = feats[0].shape[1]
    return pl.pallas_call(
        functools.partial(outer_kernel, count),
        out_shape=jax.ShapeDtypeStruct((tok, 256 * count), BF16),
        in_specs=[VMEM] * (3 * count),
        out_specs=VMEM,
        compiler_params=pltpu.CompilerParams(vmem_limit_bytes=24 * 2**20),
        cost_estimate=pl.CostEstimate(
            flops=3 * 10**8 * count, bytes_accessed=2**20 * count, transcendentals=0
        ),
        name="outer_stage",
    )(*prefixes, *feats, *parts)


def fetch_kernel(w_hbm, out, sem):
    own = lax.axis_index("head")
    cols = pl.ds(pl.multiple_of(own * 1024, 1024), 1024)

    def copy(half, s):
        start = pl.multiple_of((own ^ half) * 1024 + quarter_of(OUT_STEPS[s]) * 256, 256)
        return pltpu.make_async_copy(
            w_hbm.at[pl.ds(start, 256), cols],
            out.at[half, pl.ds(s * 256, 256)],
            sem.at[half * 4 + s],
        )

    pieces = [copy(half, s) for half in range(2) for s in range(4)]
    for piece in pieces:
        piece.start()
    for piece in pieces:
        piece.wait()


def fetch_stage(w_out):
    return pl.pallas_call(
        fetch_kernel,
        out_shape=jax.ShapeDtypeStruct((2, 1024, 1024), BF16),
        in_specs=[ANY],
        out_specs=VMEM,
        scratch_shapes=[pltpu.SemaphoreType.DMA((8,))],
        compiler_params=pltpu.CompilerParams(vmem_limit_bytes=FETCH_LIMIT),
        cost_estimate=pl.CostEstimate(
            flops=10**9, bytes_accessed=8 * 2**20, transcendentals=0
        ),
        name="fetch_stage",
    )(w_out)


def out_kernel(half, a_ref, b_ref, w_ref, *rest):
    wide = a_ref.shape[1]
    blocks = a_ref.shape[0] // CHUNK
    for c in range(blocks):
        rows = slice(c * CHUNK, (c + 1) * CHUNK)
        part = mm(a_ref[rows], w_ref[half, :wide]) + mm(b_ref[rows], w_ref[half, wide:])
        if half == 0:
            rest[0][rows] = part
        else:
            acc, out, stage, sem = rest
            stage[rows] = (part + acc[rows]).astype(BF16)
            pltpu.make_async_copy(stage.at[rows], out.at[rows], sem.at[c]).start()
    if half == 1:
        acc, out, stage, sem = rest
        for c in range(blocks):
            rows = slice(c * CHUNK, (c + 1) * CHUNK)
            pltpu.make_async_copy(stage.at[rows], out.at[rows], sem.at[c]).wait()


def out_stage(half, most, rest, columns, acc=None):
    tok = most.shape[0]
    first = half == 0
    return pl.pallas_call(
        functools.partial(out_kernel, half),
        out_shape=jax.ShapeDtypeStruct((tok, 1024), F32 if first else BF16),
        in_specs=[VMEM] * (3 if first else 4),
        out_specs=VMEM if first else ANY,
        scratch_shapes=[]
        if first
        else [pltpu.VMEM((tok, 1024), BF16), pltpu.SemaphoreType.DMA((tok // CHUNK,))],
        compiler_params=pltpu.CompilerParams(vmem_limit_bytes=OUT_LIMIT),
        cost_estimate=pl.CostEstimate(
            flops=2 * 10**9, bytes_accessed=8 * 2**20, transcendentals=0
        ),
        name="out_stage",
    )(*([most, rest, columns] + ([] if first else [acc])))


def partner(x, axis, step):
    pairs = [(i, i ^ step) for i in range(4)]
    return lax.ppermute(x, axis, pairs)


def total_kernel(p0, p1, p2, p3, out):
    total = p0[...].astype(F32) + p1[...].astype(F32)
    out[...] = (total + p2[...].astype(F32) + p3[...].astype(F32)).astype(BF16)


def level_kernel(axis, own, g0, g1, g2, base_in, total, base):
    at = lax.axis_index(axis)
    run, before = (own[...].astype(F32), jnp.zeros(own.shape, F32))
    if base_in is not None:
        before = base_in[...]
    for step, ref in zip(STEPS, (g0, g1, g2)):
        got = ref[...].astype(F32)
        run = run + got
        before = before + got * ((at ^ step) < at).astype(F32)
    if total is not None:
        total[...] = run.astype(BF16)
    base[...] = before


def spread_kernel(own, g0, g1, g2, base_in, p0, p1, p2, p3, o0, o1, o2, o3, base):
    level_kernel(SEQ[0], own, g0, g1, g2, base_in, None, base)
    at = lax.axis_index(SEQ[2])
    parts = [p[...].astype(F32) for p in (p0, p1, p2, p3)]
    for mine, out in zip(SLOTS, (o0, o1, o2, o3)):
        run = base[...]
        for step, part in zip(SLOTS, parts):
            run = run + part * ((at ^ step) < (at ^ mine)).astype(F32)
        out[...] = run.astype(BF16)


def small_call(kernel, outs, *args, scratch=(), after=()):
    shape = args[0].shape
    return pl.pallas_call(
        kernel,
        out_shape=[jax.ShapeDtypeStruct(shape, kind) for kind in outs],
        in_specs=[VMEM] * len(args) + [ANY] * len(after),
        out_specs=[VMEM] * len(outs),
        scratch_shapes=list(scratch),
        compiler_params=pltpu.CompilerParams(vmem_limit_bytes=4 * 2**20),
        cost_estimate=pl.CostEstimate(flops=10**6, bytes_accessed=2**20, transcendentals=0),
    )(*args, *after)


def middle_kernel(own, g0, g1, g2, columns, total, base):
    level_kernel(SEQ[1], own, g0, g1, g2, None, total, base)


def exclusive_prefix(states, columns):
    parts = [states[0]] + [partner(state, SEQ[2], step) for step, state in zip(STEPS, states[1:])]
    (low,) = small_call(total_kernel, [BF16], *parts)
    got = [partner(low, SEQ[1], step) for step in STEPS]
    total, base = small_call(middle_kernel, [BF16, F32], low, *got, after=[columns])
    got = [partner(total, SEQ[0], step) for step in STEPS]
    scratch = [pltpu.VMEM(low.shape, F32)]
    outs = small_call(spread_kernel, [BF16] * 4, total, *got, base, *parts, scratch=scratch)
    back = {0: outs[0]}
    for step, out in zip(STEPS, outs[1:]):
        back[step] = partner(out, SEQ[2], step)
    return back


def per_device(tokens, w_query, w_key, w_value, w_out):
    table = jnp.asarray(feature_tables())
    q, kt, val, local, *states = head_stage(tokens, w_key, w_query, w_value)
    columns = fetch_stage(w_out)
    back = exclusive_prefix(states, columns)
    inner = {}
    for slot, step in enumerate(SLOTS):
        inner[step] = inner_stage(slot, q, kt, val, local, table)

    def outer(steps):
        return outer_stage(
            [back[step] for step in steps],
            [inner[step][0] for step in steps],
            [inner[step][1] for step in steps],
        )

    most, rest = (outer(OUT_STEPS[:3]), outer(OUT_STEPS[3:]))
    swap = [(0, 1), (1, 0)]
    other_most = lax.ppermute(most, "head", swap)
    other_rest = lax.ppermute(rest, "head", swap)
    acc = out_stage(0, most, rest, columns)
    return out_stage(1, other_most, other_rest, columns, acc)


def solution(mesh):
    split = Mesh(
        mesh.devices.reshape(4, 4, 4, mesh.shape["head"]), ("seq_0", "seq_1", "seq_2", "head")
    )
    in_specs = (P(SEQ, None), P(None, "head"), P(None, "head"), P(None, "head"), P())
    out_specs = P(SEQ, "head")
    return jax.shard_map(
        per_device, mesh=split, in_specs=in_specs, out_specs=out_specs, check_vma=False
    )
```

```python
import functools

import jax
import jax.numpy as jnp
import numpy as np
from jax import lax
from jax.experimental import pallas as pl
from jax.experimental.pallas import tpu as pltpu
from jax.sharding import Mesh
from jax.sharding import PartitionSpec as P


ROWS = 160
CHUNK = 256
SEQ = ("seq_0", "seq_1", "seq_2")
STEPS = (2, 1, 3)
MIB = 2**20
HEAD_LIMIT, FETCH_LIMIT, OUT_LIMIT = (48 * MIB, 44 * MIB, 20 * MIB)
SLOTS = (0, 2, 1, 3)
OUT_STEPS = (0, 1, 3, 2)
GROUPS = ((0,), (1, 3), (2,))
F32, BF16 = (jnp.float32, jnp.bfloat16)
VMEM = pl.BlockSpec(memory_space=pltpu.VMEM)
SMEM = pl.BlockSpec(memory_space=pltpu.SMEM)
ANY = pl.BlockSpec(memory_space=pl.ANY)
NN = (((1,), (0,)), ((), ()))


def mm(a, b):
    return lax.dot_general(a, b, NN, preferred_element_type=F32)


def quarter_of(step):
    return lax.axis_index(SEQ[2]) ^ step


def feature_tables():
    first, second, scale = ([-1] * ROWS, [-1] * ROWS, [0.0] * ROWS)
    for d in range(9):
        for a in range(16 if d < 8 else 8):
            row = 16 * d + a
            first[row], second[row] = (a, (a + d) % 16)
            scale[row] = 1.0 / 32.0 if d == 0 else 1.0 / 16.0
    for a in range(16):
        first[136 + a], scale[136 + a] = (a, 0.25)
    scale[152] = 1.0
    table = np.zeros((8, ROWS), np.float32)
    table[0], table[1], table[2] = (first, second, scale)
    table[3, 152] = 1.0
    table[4, 136:153] = scale[136:153]
    return table


def key_features(u):
    tok = u.shape[1]
    blocks = [u * u]
    for d in range(1, 9):
        blocks.append(u * pltpu.roll(u, 16 - d, 0))
    blocks[8] = blocks[8][:8]
    row = lax.broadcasted_iota(jnp.int32, (8, tok), 0)
    tail = jnp.where(row == 0, 1.0, 0.0)
    return jnp.concatenate(blocks + [u, tail], axis=0).astype(BF16)


def norm_rows(norm):
    top = jnp.transpose(norm[:128])[:1]
    rest = jnp.concatenate([norm[128:], jnp.zeros((96, 128), F32)], axis=0)
    low = jnp.transpose(rest)[:1]
    row = lax.broadcasted_iota(jnp.int32, (8, 128), 0)
    return jnp.where(row == 1, top, jnp.where(row == 2, low, 0.0))


def head_kernel(
    x_hbm, wk_hbm, wq_hbm, wv_hbm,
    q_out, kt_out, val_out, local_out, s0, s1, s2, s3,
    x, wkq, wv, acc, kt, x_sem, w_sem, v_sem,
):
    tok, width = x.shape
    cuts = 4
    cut = width // cuts
    kd = wk_hbm.shape[1]

    def wcopy(j, src, half):
        rows = pl.ds(j * cut, cut)
        return pltpu.make_async_copy(
            src.at[rows], wkq.at[rows, pl.ds(half * kd, kd)], w_sem.at[2 * j + half]
        )

    def xcopy(j):
        cols = pl.ds(j * cut, cut)
        return pltpu.make_async_copy(x_hbm.at[:, cols], x.at[:, cols], x_sem.at[j])

    def vcopy(s):
        start = pl.multiple_of(quarter_of(SLOTS[s]) * 256, 256)
        return pltpu.make_async_copy(
            wv_hbm.at[:, pl.ds(start, 256)],
            wv.at[s // 2, :, pl.ds(s % 2 * 256, 256)],
            v_sem.at[s],
        )

    for j in range(cuts):
        wcopy(j, wk_hbm, 0).start()
        wcopy(j, wq_hbm, 1).start()
        xcopy(j).start()
    for s in range(4):
        vcopy(s).start()
    for j in range(cuts):
        wcopy(j, wk_hbm, 0).wait()
        wcopy(j, wq_hbm, 1).wait()
        xcopy(j).wait()
        cols = slice(j * cut, (j + 1) * cut)
        for rows in (slice(0, tok // 2), slice(tok // 2, tok)):
            part = mm(x[rows, cols], wkq[cols])
            acc[rows] = part if j == 0 else acc[rows] + part
    q_out[...] = acc[:, kd:].astype(BF16)
    keys = jnp.transpose(acc[:, :kd].astype(BF16).astype(F32))
    kt[...] = keys
    kt_out[...] = keys.astype(BF16)
    ones = jnp.ones((CHUNK, 128), BF16)
    for s, state in enumerate((s0, s1, s2, s3)):
        if s % 2 == 0:
            vcopy(s).wait()
            vcopy(s + 1).wait()
            pair = mm(x[...], wv[s // 2]).astype(BF16)
        val = pair[:, s % 2 * 256 : s % 2 * 256 + 256]
        val_out[s] = val
        for h in range(2):
            at = pl.multiple_of((quarter_of(SLOTS[s]) * 2 + h) * 16, 16)
            feat = key_features(kt[pl.ds(at, 16), :])
            run = None
            for c in range(tok // CHUNK):
                rows = slice(c * CHUNK, (c + 1) * CHUNK)
                right = jnp.concatenate([val[rows, h * 128 : (h + 1) * 128], ones], axis=1)
                part = mm(feat[:, rows], right)
                run = part if c == 0 else run + part
                if c < tok // CHUNK - 1:
                    local_out[s, h, c] = run.astype(BF16)
            state[h, :152] = run[:152, :128].astype(BF16)
            extra = norm_rows(run[:, 128:])
            row = lax.broadcasted_iota(jnp.int32, (8, 128), 0)
            state[h, 152:] = jnp.where(row == 0, run[152:, :128], extra).astype(BF16)


def head_stage(tokens, w_key, w_query, w_value):
    tok, width = tokens.shape
    kd = w_key.shape[1]
    chunks = tok // CHUNK
    shape = jax.ShapeDtypeStruct
    return pl.pallas_call(
        head_kernel,
        out_shape=[
            shape((tok, kd), BF16),
            shape((kd, tok), BF16),
            shape((4, tok, 256), BF16),
            shape((4, 2, chunks - 1, ROWS, 256), BF16),
        ]
        + [shape((2, ROWS, 128), BF16)] * 4,
        in_specs=[ANY] * 4,
        out_specs=[VMEM] * 8,
        scratch_shapes=[
            pltpu.VMEM((tok, width), BF16),
            pltpu.VMEM((width, 2 * kd), BF16),
            pltpu.VMEM((2, width, 512), BF16),
            pltpu.VMEM((tok, 2 * kd), F32),
            pltpu.VMEM((kd, tok), F32),
            pltpu.SemaphoreType.DMA((4,)),
            pltpu.SemaphoreType.DMA((8,)),
            pltpu.SemaphoreType.DMA((4,)),
        ],
        compiler_params=pltpu.CompilerParams(vmem_limit_bytes=HEAD_LIMIT),
        cost_estimate=pl.CostEstimate(
            flops=6 * 10**9, bytes_accessed=12 * 2**20, transcendentals=0
        ),
        name="head_stage",
    )(tokens, w_key, w_query, w_value)


def inner_kernel(slot, q_ref, kt_ref, val_ref, local_ref, table_ref, feat_out, part_out):
    tok = q_ref.shape[0]
    ones = jnp.ones((CHUNK, 128), BF16)
    below = lax.broadcasted_iota(jnp.int32, (CHUNK, CHUNK), 0) >= lax.broadcasted_iota(
        jnp.int32, (CHUNK, CHUNK), 1
    )
    first, second, scale = (table_ref[0:1], table_ref[1:2], table_ref[2:3])
    add_first, add_second = (table_ref[3:4], table_ref[4:5])
    entry = lax.broadcasted_iota(jnp.int32, (128, ROWS), 0).astype(F32)
    lane = lax.broadcasted_iota(jnp.int32, (CHUNK, 128), 1)
    for h in range(2):
        at = (quarter_of(SLOTS[slot]) * 2 + h) * 16
        base = at.astype(F32)
        pick_first = jnp.where((entry == first + base) & (first >= 0), 1.0, 0.0).astype(BF16)
        pick_second = jnp.where((entry == second + base) & (second >= 0), scale, 0.0).astype(BF16)
        mine = (lane >= at) & (lane < at + 16)
        for c in range(tok // CHUNK):
            rows = slice(c * CHUNK, (c + 1) * CHUNK)
            q = q_ref[rows]
            feat = (mm(q, pick_first) + add_first) * (mm(q, pick_second) + add_second)
            feat = feat.astype(BF16)
            feat_out[h, rows] = feat
            own = jnp.where(mine, q.astype(F32) * 0.25, 0.0).astype(BF16)
            s = mm(own, kt_ref[:, rows])
            taylor = jnp.where(below, (0.5 * s + 1.0) * s + 1.0, 0.0).astype(BF16)
            right = jnp.concatenate([val_ref[0, rows, h * 128 : (h + 1) * 128], ones], axis=1)
            part = mm(taylor, right)
            if c > 0:
                part = part + mm(feat, local_ref[0, h, c - 1])
            part_out[h, rows] = part


def inner_stage(slot, q, kt, val, local, table):
    tok = q.shape[0]
    shape = jax.ShapeDtypeStruct
    return pl.pallas_call(
        functools.partial(inner_kernel, slot),
        grid=(1,),
        out_shape=[shape((2, tok, ROWS), BF16), shape((2, tok, 256), F32)],
        in_specs=[
            pl.BlockSpec(q.shape, lambda i: (0, 0)),
            pl.BlockSpec(kt.shape, lambda i: (0, 0)),
            pl.BlockSpec((1,) + val.shape[1:], lambda i: (slot, 0, 0)),
            pl.BlockSpec((1,) + local.shape[1:], lambda i: (slot, 0, 0, 0, 0)),
            pl.BlockSpec(table.shape, lambda i: (0, 0)),
        ],
        out_specs=[
            pl.BlockSpec((2, tok, ROWS), lambda i: (0, 0, 0)),
            pl.BlockSpec((2, tok, 256), lambda i: (0, 0, 0)),
        ],
        compiler_params=pltpu.CompilerParams(vmem_limit_bytes=16 * 2**20),
        cost_estimate=pl.CostEstimate(
            flops=2 * 10**9, bytes_accessed=4 * 2**20, transcendentals=0
        ),
        name="inner_stage",
    )(q, kt, val, local, table)


def outer_kernel(count, *refs):
    prefixes, feats, parts, out = (
        refs[:count], refs[count : 2 * count], refs[2 * count : 3 * count], refs[3 * count]
    )
    for i in range(count):
        for h in range(2):
            low = prefixes[i][h]
            wide = low[152:].astype(F32)
            top = jnp.transpose(jnp.broadcast_to(wide[1:2], (128, 128)))
            rest = jnp.transpose(jnp.broadcast_to(wide[2:3], (128, 128)))[:32]
            norm = jnp.concatenate([top, rest], axis=0).astype(BF16)
            right = jnp.concatenate([low, norm], axis=1)
            both = mm(feats[i][h], right) + parts[i][h]
            cols = slice(i * 256 + h * 128, i * 256 + (h + 1) * 128)
            out[:, cols] = (both[:, :128] / both[:, 128:]).astype(BF16)


def outer_stage(prefixes, feats, parts):
    count = len(prefixes)
    tok = feats[0].shape[1]
    return pl.pallas_call(
        functools.partial(outer_kernel, count),
        out_shape=jax.ShapeDtypeStruct((tok, 256 * count), BF16),
        in_specs=[VMEM] * (3 * count),
        out_specs=VMEM,
        compiler_params=pltpu.CompilerParams(vmem_limit_bytes=24 * 2**20),
        cost_estimate=pl.CostEstimate(
            flops=3 * 10**8 * count, bytes_accessed=2**20 * count, transcendentals=0
        ),
        name="outer_stage",
    )(*prefixes, *feats, *parts)


def fetch_kernel(w_hbm, out, sem):
    own = lax.axis_index("head")
    cols = pl.ds(pl.multiple_of(own * 1024, 1024), 1024)

    def copy(half, s):
        start = pl.multiple_of((own ^ half) * 1024 + quarter_of(OUT_STEPS[s]) * 256, 256)
        return pltpu.make_async_copy(
            w_hbm.at[pl.ds(start, 256), cols],
            out.at[half, pl.ds(s * 256, 256)],
            sem.at[half * 4 + s],
        )

    pieces = [copy(half, s) for half in range(2) for s in range(4)]
    for piece in pieces:
        piece.start()
    for piece in pieces:
        piece.wait()


def fetch_stage(w_out):
    return pl.pallas_call(
        fetch_kernel,
        out_shape=jax.ShapeDtypeStruct((2, 1024, 1024), BF16),
        in_specs=[ANY],
        out_specs=VMEM,
        scratch_shapes=[pltpu.SemaphoreType.DMA((8,))],
        compiler_params=pltpu.CompilerParams(vmem_limit_bytes=FETCH_LIMIT),
        cost_estimate=pl.CostEstimate(
            flops=10**9, bytes_accessed=8 * 2**20, transcendentals=0
        ),
        name="fetch_stage",
    )(w_out)


def out_kernel(places, last, *refs):
    count = len(places)
    groups, (w_ref, *rest) = (refs[:count], refs[count:])
    tok = groups[0].shape[0]
    blocks = tok // CHUNK
    if last:
        acc, out, stage, sem = rest
        copies = []
        for c in range(blocks):
            rows = pl.ds(c * CHUNK, CHUNK)
            copies.append(pltpu.make_async_copy(stage.at[rows], out.at[rows], sem.at[c]))
    else:
        acc, out = (None, rest[0]) if len(rest) == 1 else rest
    for c in range(blocks):
        rows = slice(c * CHUNK, (c + 1) * CHUNK)
        part = None if acc is None else acc[rows]
        for group, (half, start, width) in zip(groups, places):
            more = mm(group[rows], w_ref[half, start : start + width])
            part = more if part is None else part + more
        if last:
            stage[rows] = part.astype(BF16)
            copies[c].start()
        else:
            out[rows] = part
    if last:
        for copy in copies:
            copy.wait()


def out_stage(groups, places, columns, acc=None, last=False):
    tok = groups[0].shape[0]
    args = [*groups, columns] + ([] if acc is None else [acc])
    depth = sum(width for _, _, width in places)
    return pl.pallas_call(
        functools.partial(out_kernel, places, last),
        out_shape=jax.ShapeDtypeStruct((tok, 1024), BF16 if last else F32),
        in_specs=[VMEM] * len(args),
        out_specs=ANY if last else VMEM,
        scratch_shapes=[pltpu.VMEM((tok, 1024), BF16), pltpu.SemaphoreType.DMA((tok // CHUNK,))]
        if last
        else [],
        compiler_params=pltpu.CompilerParams(vmem_limit_bytes=OUT_LIMIT),
        cost_estimate=pl.CostEstimate(
            flops=2 * tok * 1024 * depth, bytes_accessed=2**20, transcendentals=0
        ),
        name="out_stage",
    )(*args)


def partner(x, axis, step):
    pairs = [(i, i ^ step) for i in range(4)]
    return lax.ppermute(x, axis, pairs)


def total_kernel(p0, p1, p2, p3, out):
    total = p0[...].astype(F32) + p1[...].astype(F32)
    out[...] = (total + p2[...].astype(F32) + p3[...].astype(F32)).astype(BF16)


def level_kernel(axis, own, g0, g1, g2, base_in, total, base):
    at = lax.axis_index(axis)
    run, before = (own[...].astype(F32), jnp.zeros(own.shape, F32))
    if base_in is not None:
        before = base_in[...]
    for step, ref in zip(STEPS, (g0, g1, g2)):
        got = ref[...].astype(F32)
        run = run + got
        before = before + got * ((at ^ step) < at).astype(F32)
    if total is not None:
        total[...] = run.astype(BF16)
    base[...] = before


def spread_kernel(own, g0, g1, g2, base_in, p0, p1, p2, p3, o0, o1, o2, o3, base):
    level_kernel(SEQ[0], own, g0, g1, g2, base_in, None, base)
    at = lax.axis_index(SEQ[2])
    parts = [p[...].astype(F32) for p in (p0, p1, p2, p3)]
    for mine, out in zip(SLOTS, (o0, o1, o2, o3)):
        run = base[...]
        for step, part in zip(SLOTS, parts):
            run = run + part * ((at ^ step) < (at ^ mine)).astype(F32)
        out[...] = run.astype(BF16)


def small_call(kernel, outs, *args, scratch=(), after=()):
    shape = args[0].shape
    return pl.pallas_call(
        kernel,
        out_shape=[jax.ShapeDtypeStruct(shape, kind) for kind in outs],
        in_specs=[VMEM] * len(args) + [ANY] * len(after),
        out_specs=[VMEM] * len(outs),
        scratch_shapes=list(scratch),
        compiler_params=pltpu.CompilerParams(vmem_limit_bytes=4 * 2**20),
        cost_estimate=pl.CostEstimate(flops=10**6, bytes_accessed=2**20, transcendentals=0),
    )(*args, *after)


def middle_kernel(own, g0, g1, g2, columns, total, base):
    level_kernel(SEQ[1], own, g0, g1, g2, None, total, base)


def exclusive_prefix(states, columns):
    parts = [states[0]] + [partner(state, SEQ[2], step) for step, state in zip(STEPS, states[1:])]
    (low,) = small_call(total_kernel, [BF16], *parts)
    got = [partner(low, SEQ[1], step) for step in STEPS]
    total, base = small_call(middle_kernel, [BF16, F32], low, *got, after=[columns])
    got = [partner(total, SEQ[0], step) for step in STEPS]
    scratch = [pltpu.VMEM(low.shape, F32)]
    outs = small_call(spread_kernel, [BF16] * 4, total, *got, base, *parts, scratch=scratch)
    back = {0: outs[0]}
    for step, out in zip(STEPS, outs[1:]):
        back[step] = partner(out, SEQ[2], step)
    return back


def per_device(tokens, w_query, w_key, w_value, w_out):
    tokens, w_query, w_key, w_value, w_out = (
        pltpu.with_memory_space_constraint(x, pltpu.HBM)
        for x in (tokens, w_query, w_key, w_value, w_out)
    )
    table = jnp.asarray(feature_tables())
    q, kt, val, local, *states = head_stage(tokens, w_key, w_query, w_value)
    columns = fetch_stage(w_out)
    back = exclusive_prefix(states, columns)
    inner = {}
    for slot, step in enumerate(SLOTS):
        inner[step] = inner_stage(slot, q, kt, val, local, table)

    def outer(steps):
        return outer_stage(
            [back[step] for step in steps],
            [inner[step][0] for step in steps],
            [inner[step][1] for step in steps],
        )

    places, start = ([], 0)
    for steps in GROUPS:
        places.append((start, 256 * len(steps)))
        start += 256 * len(steps)
    own, other = ([], [])
    for steps in GROUPS:
        own.append(outer(steps))
        other.append(lax.ppermute(own[-1], "head", [(0, 1), (1, 0)]))
    mine = [(0, *place) for place in places]
    theirs = [(1, *place) for place in places]
    acc = out_stage(own[:1], mine[:1], columns)
    acc = out_stage([*own[1:], other[0]], (*mine[1:], theirs[0]), columns, acc)
    return out_stage(other[1:], theirs[1:], columns, acc, last=True)


def solution(mesh):
    split = Mesh(
        mesh.devices.reshape(4, 4, 4, mesh.shape["head"]), ("seq_0", "seq_1", "seq_2", "head")
    )
    in_specs = (P(SEQ, None), P(None, "head"), P(None, "head"), P(None, "head"), P())
    out_specs = P(SEQ, "head")
    return jax.shard_map(
        per_device, mesh=split, in_specs=in_specs, out_specs=out_specs, check_vma=False
    )
```

```python
import functools

import jax
import jax.numpy as jnp
import numpy as np
from jax import lax
from jax.experimental import pallas as pl
from jax.experimental.pallas import tpu as pltpu
from jax.sharding import Mesh
from jax.sharding import PartitionSpec as P


ROWS = 160
CHUNK = 256
SEQ = ("seq_0", "seq_1", "seq_2")
STEPS = (2, 1, 3)
MIB = 2**20
HEAD_LIMIT, FETCH_LIMIT, OUT_LIMIT = (48 * MIB, 44 * MIB, 20 * MIB)
SLOTS = (0, 2, 1, 3)
OUT_STEPS = (0, 2, 1, 3)
GROUPS = ((0,), (2, 1), (3,))
F32, BF16 = (jnp.float32, jnp.bfloat16)
VMEM = pl.BlockSpec(memory_space=pltpu.VMEM)
SMEM = pl.BlockSpec(memory_space=pltpu.SMEM)
ANY = pl.BlockSpec(memory_space=pl.ANY)
NN = (((1,), (0,)), ((), ()))


def mm(a, b):
    return lax.dot_general(a, b, NN, preferred_element_type=F32)


def quarter_of(step):
    return lax.axis_index(SEQ[2]) ^ step


def feature_tables():
    first, second, scale = ([-1] * ROWS, [-1] * ROWS, [0.0] * ROWS)
    for d in range(9):
        for a in range(16 if d < 8 else 8):
            row = 16 * d + a
            first[row], second[row] = (a, (a + d) % 16)
            scale[row] = 1.0 / 32.0 if d == 0 else 1.0 / 16.0
    for a in range(16):
        first[136 + a], scale[136 + a] = (a, 0.25)
    scale[152] = 1.0
    table = np.zeros((8, ROWS), np.float32)
    table[0], table[1], table[2] = (first, second, scale)
    table[3, 152] = 1.0
    table[4, 136:153] = scale[136:153]
    return table


def key_features(u):
    tok = u.shape[1]
    blocks = [u * u]
    for d in range(1, 9):
        blocks.append(u * pltpu.roll(u, 16 - d, 0))
    blocks[8] = blocks[8][:8]
    row = lax.broadcasted_iota(jnp.int32, (8, tok), 0)
    tail = jnp.where(row == 0, 1.0, 0.0)
    return jnp.concatenate(blocks + [u, tail], axis=0).astype(BF16)


def norm_rows(norm):
    top = jnp.transpose(norm[:128])[:1]
    rest = jnp.concatenate([norm[128:], jnp.zeros((96, 128), F32)], axis=0)
    low = jnp.transpose(rest)[:1]
    row = lax.broadcasted_iota(jnp.int32, (8, 128), 0)
    return jnp.where(row == 1, top, jnp.where(row == 2, low, 0.0))


def head_kernel(
    x_hbm, wk_hbm, wq_hbm, wv_hbm,
    q_out, kt_out, val_out, local_out, s0, s1, s2, s3,
    x, wkq, wv, acc, kt, x_sem, w_sem, v_sem,
):
    tok, width = x.shape
    cuts = 4
    cut = width // cuts
    kd = wk_hbm.shape[1]

    def wcopy(j, src, half):
        rows = pl.ds(j * cut, cut)
        return pltpu.make_async_copy(
            src.at[rows], wkq.at[rows, pl.ds(half * kd, kd)], w_sem.at[2 * j + half]
        )

    def xcopy(j):
        cols = pl.ds(j * cut, cut)
        return pltpu.make_async_copy(x_hbm.at[:, cols], x.at[:, cols], x_sem.at[j])

    def vcopy(s):
        start = pl.multiple_of(quarter_of(SLOTS[s]) * 256, 256)
        return pltpu.make_async_copy(
            wv_hbm.at[:, pl.ds(start, 256)],
            wv.at[s // 2, :, pl.ds(s % 2 * 256, 256)],
            v_sem.at[s],
        )

    for j in range(cuts):
        wcopy(j, wk_hbm, 0).start()
        wcopy(j, wq_hbm, 1).start()
        xcopy(j).start()
    for s in range(4):
        vcopy(s).start()
    for j in range(cuts):
        wcopy(j, wk_hbm, 0).wait()
        wcopy(j, wq_hbm, 1).wait()
        xcopy(j).wait()
        cols = slice(j * cut, (j + 1) * cut)
        for rows in (slice(0, tok // 2), slice(tok // 2, tok)):
            part = mm(x[rows, cols], wkq[cols])
            acc[rows] = part if j == 0 else acc[rows] + part
    q_out[...] = acc[:, kd:].astype(BF16)
    keys = jnp.transpose(acc[:, :kd].astype(BF16).astype(F32))
    kt[...] = keys
    kt_out[...] = keys.astype(BF16)
    ones = jnp.ones((CHUNK, 128), BF16)
    for s, state in enumerate((s0, s1, s2, s3)):
        if s % 2 == 0:
            vcopy(s).wait()
            vcopy(s + 1).wait()
            pair = mm(x[...], wv[s // 2]).astype(BF16)
        val = pair[:, s % 2 * 256 : s % 2 * 256 + 256]
        val_out[s] = val
        for h in range(2):
            at = pl.multiple_of((quarter_of(SLOTS[s]) * 2 + h) * 16, 16)
            feat = key_features(kt[pl.ds(at, 16), :])
            run = None
            for c in range(tok // CHUNK):
                rows = slice(c * CHUNK, (c + 1) * CHUNK)
                right = jnp.concatenate([val[rows, h * 128 : (h + 1) * 128], ones], axis=1)
                part = mm(feat[:, rows], right)
                run = part if c == 0 else run + part
                if c < tok // CHUNK - 1:
                    local_out[s, h, c] = run.astype(BF16)
            state[h, :152] = run[:152, :128].astype(BF16)
            extra = norm_rows(run[:, 128:])
            row = lax.broadcasted_iota(jnp.int32, (8, 128), 0)
            state[h, 152:] = jnp.where(row == 0, run[152:, :128], extra).astype(BF16)


def head_stage(tokens, w_key, w_query, w_value):
    tok, width = tokens.shape
    kd = w_key.shape[1]
    chunks = tok // CHUNK
    shape = jax.ShapeDtypeStruct
    return pl.pallas_call(
        head_kernel,
        out_shape=[
            shape((tok, kd), BF16),
            shape((kd, tok), BF16),
            shape((4, tok, 256), BF16),
            shape((4, 2, chunks - 1, ROWS, 256), BF16),
        ]
        + [shape((2, ROWS, 128), BF16)] * 4,
        in_specs=[ANY] * 4,
        out_specs=[VMEM] * 8,
        scratch_shapes=[
            pltpu.VMEM((tok, width), BF16),
            pltpu.VMEM((width, 2 * kd), BF16),
            pltpu.VMEM((2, width, 512), BF16),
            pltpu.VMEM((tok, 2 * kd), F32),
            pltpu.VMEM((kd, tok), F32),
            pltpu.SemaphoreType.DMA((4,)),
            pltpu.SemaphoreType.DMA((8,)),
            pltpu.SemaphoreType.DMA((4,)),
        ],
        compiler_params=pltpu.CompilerParams(vmem_limit_bytes=HEAD_LIMIT),
        cost_estimate=pl.CostEstimate(
            flops=6 * 10**9, bytes_accessed=12 * 2**20, transcendentals=0
        ),
        name="head_stage",
    )(tokens, w_key, w_query, w_value)


def inner_kernel(slot, h, q_ref, kt_ref, val_ref, local_ref, table_ref, feat_out, part_out):
    tok = q_ref.shape[0]
    ones = jnp.ones((CHUNK, 128), BF16)
    below = lax.broadcasted_iota(jnp.int32, (CHUNK, CHUNK), 0) >= lax.broadcasted_iota(
        jnp.int32, (CHUNK, CHUNK), 1
    )
    first, second, scale = (table_ref[0:1], table_ref[1:2], table_ref[2:3])
    add_first, add_second = (table_ref[3:4], table_ref[4:5])
    entry = lax.broadcasted_iota(jnp.int32, (128, ROWS), 0).astype(F32)
    lane = lax.broadcasted_iota(jnp.int32, (CHUNK, 128), 1)
    at = (quarter_of(SLOTS[slot]) * 2 + h) * 16
    base = at.astype(F32)
    pick_first = jnp.where((entry == first + base) & (first >= 0), 1.0, 0.0).astype(BF16)
    pick_second = jnp.where((entry == second + base) & (second >= 0), scale, 0.0).astype(BF16)
    mine = (lane >= at) & (lane < at + 16)
    for c in range(tok // CHUNK):
        rows = slice(c * CHUNK, (c + 1) * CHUNK)
        q = q_ref[rows]
        feat = (mm(q, pick_first) + add_first) * (mm(q, pick_second) + add_second)
        feat = feat.astype(BF16)
        feat_out[rows] = feat
        own = jnp.where(mine, q.astype(F32) * 0.25, 0.0).astype(BF16)
        s = mm(own, kt_ref[:, rows])
        taylor = jnp.where(below, (0.5 * s + 1.0) * s + 1.0, 0.0).astype(BF16)
        right = jnp.concatenate([val_ref[slot, rows, h * 128 : (h + 1) * 128], ones], axis=1)
        part = mm(taylor, right)
        if c > 0:
            part = part + mm(feat, local_ref[slot, h, c - 1])
        part_out[rows] = part


def inner_stage(slot, h, *args):
    tok = args[0].shape[0]
    shape = jax.ShapeDtypeStruct
    return pl.pallas_call(
        functools.partial(inner_kernel, slot, h),
        out_shape=[shape((tok, ROWS), BF16), shape((tok, 256), F32)],
        in_specs=[VMEM] * 5,
        out_specs=[VMEM] * 2,
        compiler_params=pltpu.CompilerParams(vmem_limit_bytes=16 * MIB),
        cost_estimate=pl.CostEstimate(flops=10**9, bytes_accessed=2 * MIB, transcendentals=0),
        name="inner_stage",
    )(*args)


def outer_kernel(count, *refs):
    prefixes, (*inner, out) = (refs[:count], refs[count:])
    feats, parts = (inner[: 2 * count], inner[2 * count :])
    for i in range(count):
        for h in range(2):
            low = prefixes[i][h]
            wide = low[152:].astype(F32)
            top = jnp.transpose(jnp.broadcast_to(wide[1:2], (128, 128)))
            rest = jnp.transpose(jnp.broadcast_to(wide[2:3], (128, 128)))[:32]
            norm = jnp.concatenate([top, rest], axis=0).astype(BF16)
            right = jnp.concatenate([low, norm], axis=1)
            both = mm(feats[2 * i + h][...], right) + parts[2 * i + h][...]
            cols = slice(i * 256 + h * 128, i * 256 + (h + 1) * 128)
            out[:, cols] = (both[:, :128] / both[:, 128:]).astype(BF16)


def outer_stage(prefixes, feats, parts):
    count = len(prefixes)
    tok = feats[0].shape[0]
    return pl.pallas_call(
        functools.partial(outer_kernel, count),
        out_shape=jax.ShapeDtypeStruct((tok, 256 * count), BF16),
        in_specs=[VMEM] * (5 * count),
        out_specs=VMEM,
        compiler_params=pltpu.CompilerParams(vmem_limit_bytes=24 * 2**20),
        cost_estimate=pl.CostEstimate(
            flops=3 * 10**8 * count, bytes_accessed=2**20 * count, transcendentals=0
        ),
        name="outer_stage",
    )(*prefixes, *feats, *parts)


def fetch_kernel(w_hbm, out, sem):
    own = lax.axis_index("head")
    cols = pl.ds(pl.multiple_of(own * 1024, 1024), 1024)

    def copy(half, s):
        start = pl.multiple_of((own ^ half) * 1024 + quarter_of(OUT_STEPS[s]) * 256, 256)
        return pltpu.make_async_copy(
            w_hbm.at[pl.ds(start, 256), cols],
            out.at[half, pl.ds(s * 256, 256)],
            sem.at[half * 4 + s],
        )

    pieces = [copy(half, s) for half in range(2) for s in range(4)]
    for piece in pieces:
        piece.start()
    for piece in pieces:
        piece.wait()


def fetch_stage(w_out):
    return pl.pallas_call(
        fetch_kernel,
        out_shape=jax.ShapeDtypeStruct((2, 1024, 1024), BF16),
        in_specs=[ANY],
        out_specs=VMEM,
        scratch_shapes=[pltpu.SemaphoreType.DMA((8,))],
        compiler_params=pltpu.CompilerParams(vmem_limit_bytes=FETCH_LIMIT),
        cost_estimate=pl.CostEstimate(
            flops=10**9, bytes_accessed=8 * 2**20, transcendentals=0
        ),
        name="fetch_stage",
    )(w_out)


def out_kernel(places, last, *refs):
    count = len(places)
    groups, (w_ref, *rest) = (refs[:count], refs[count:])
    tok = groups[0].shape[0]
    blocks = tok // CHUNK
    if last:
        acc, out, stage, sem = rest
        copies = []
        for c in range(blocks):
            rows = pl.ds(c * CHUNK, CHUNK)
            copies.append(pltpu.make_async_copy(stage.at[rows], out.at[rows], sem.at[c]))
    else:
        acc, out = (None, rest[0]) if len(rest) == 1 else rest
    for c in range(blocks):
        rows = slice(c * CHUNK, (c + 1) * CHUNK)
        part = None if acc is None else acc[rows]
        for group, (half, start, width) in zip(groups, places):
            more = mm(group[rows], w_ref[half, start : start + width])
            part = more if part is None else part + more
        if last:
            stage[rows] = part.astype(BF16)
            copies[c].start()
        else:
            out[rows] = part
    if last:
        for copy in copies:
            copy.wait()


def out_stage(groups, places, columns, acc=None, last=False):
    tok = groups[0].shape[0]
    args = [*groups, columns] + ([] if acc is None else [acc])
    depth = sum(width for _, _, width in places)
    return pl.pallas_call(
        functools.partial(out_kernel, places, last),
        out_shape=jax.ShapeDtypeStruct((tok, 1024), BF16 if last else F32),
        in_specs=[VMEM] * len(args),
        out_specs=ANY if last else VMEM,
        scratch_shapes=[pltpu.VMEM((tok, 1024), BF16), pltpu.SemaphoreType.DMA((tok // CHUNK,))]
        if last
        else [],
        compiler_params=pltpu.CompilerParams(vmem_limit_bytes=OUT_LIMIT),
        cost_estimate=pl.CostEstimate(
            flops=2 * tok * 1024 * depth, bytes_accessed=2**20, transcendentals=0
        ),
        name="out_stage",
    )(*args)


def partner(x, axis, step):
    pairs = [(i, i ^ step) for i in range(4)]
    return lax.ppermute(x, axis, pairs)


def total_kernel(p0, p1, p2, p3, out):
    total = p0[...].astype(F32) + p1[...].astype(F32)
    out[...] = (total + p2[...].astype(F32) + p3[...].astype(F32)).astype(BF16)


def level_kernel(axis, own, g0, g1, g2, base_in, total, base):
    at = lax.axis_index(axis)
    run, before = (own[...].astype(F32), jnp.zeros(own.shape, F32))
    if base_in is not None:
        before = base_in[...]
    for step, ref in zip(STEPS, (g0, g1, g2)):
        got = ref[...].astype(F32)
        run = run + got
        before = before + got * ((at ^ step) < at).astype(F32)
    if total is not None:
        total[...] = run.astype(BF16)
    base[...] = before


def spread_kernel(own, g0, g1, g2, base_in, p0, p1, p2, p3, o0, o1, o2, o3, base):
    level_kernel(SEQ[0], own, g0, g1, g2, base_in, None, base)
    at = lax.axis_index(SEQ[2])
    parts = [p[...].astype(F32) for p in (p0, p1, p2, p3)]
    for mine, out in zip(SLOTS, (o0, o1, o2, o3)):
        run = base[...]
        for step, part in zip(SLOTS, parts):
            run = run + part * ((at ^ step) < (at ^ mine)).astype(F32)
        out[...] = run.astype(BF16)


def small_call(kernel, outs, *args, scratch=(), after=()):
    shape = args[0].shape
    return pl.pallas_call(
        kernel,
        out_shape=[jax.ShapeDtypeStruct(shape, kind) for kind in outs],
        in_specs=[VMEM] * len(args) + [ANY] * len(after),
        out_specs=[VMEM] * len(outs),
        scratch_shapes=list(scratch),
        compiler_params=pltpu.CompilerParams(vmem_limit_bytes=4 * 2**20),
        cost_estimate=pl.CostEstimate(flops=10**6, bytes_accessed=2**20, transcendentals=0),
    )(*args, *after)


def middle_kernel(own, g0, g1, g2, columns, total, base):
    level_kernel(SEQ[1], own, g0, g1, g2, None, total, base)


def exclusive_prefix(states, columns):
    parts = [states[0]] + [partner(state, SEQ[2], step) for step, state in zip(STEPS, states[1:])]
    (low,) = small_call(total_kernel, [BF16], *parts)
    got = [partner(low, SEQ[1], step) for step in STEPS]
    total, base = small_call(middle_kernel, [BF16, F32], low, *got, after=[columns])
    got = [partner(total, SEQ[0], step) for step in STEPS]
    scratch = [pltpu.VMEM(low.shape, F32)]
    outs = small_call(spread_kernel, [BF16] * 4, total, *got, base, *parts, scratch=scratch)
    back = {0: outs[0]}
    for step, out in zip(STEPS, outs[1:]):
        back[step] = partner(out, SEQ[2], step)
    return back


def per_device(tokens, w_query, w_key, w_value, w_out):
    tokens, w_query, w_key, w_value, w_out = (
        pltpu.with_memory_space_constraint(x, pltpu.HBM)
        for x in (tokens, w_query, w_key, w_value, w_out)
    )
    table = jnp.asarray(feature_tables())
    q, kt, val, local, *states = head_stage(tokens, w_key, w_query, w_value)
    columns = fetch_stage(w_out)
    back = exclusive_prefix(states, columns)
    inner = {}
    for slot, step in enumerate(SLOTS):
        for h in range(2):
            inner[step, h] = inner_stage(slot, h, q, kt, val, local, table)

    def outer(steps):
        return outer_stage(
            [back[step] for step in steps],
            [inner[step, h][0] for step in steps for h in range(2)],
            [inner[step, h][1] for step in steps for h in range(2)],
        )

    places, start = ([], 0)
    for steps in GROUPS:
        places.append((start, 256 * len(steps)))
        start += 256 * len(steps)
    own, other = ([], [])
    for steps in GROUPS:
        own.append(outer(steps))
        other.append(lax.ppermute(own[-1], "head", [(0, 1), (1, 0)]))
    mine = [(0, *place) for place in places]
    theirs = [(1, *place) for place in places]
    acc = out_stage(own[:1], mine[:1], columns)
    acc = out_stage([*own[1:], other[0]], (*mine[1:], theirs[0]), columns, acc)
    return out_stage(other[1:], theirs[1:], columns, acc, last=True)


def solution(mesh):
    split = Mesh(
        mesh.devices.reshape(4, 4, 4, mesh.shape["head"]), ("seq_0", "seq_1", "seq_2", "head")
    )
    in_specs = (P(SEQ, None), P(None, "head"), P(None, "head"), P(None, "head"), P())
    out_specs = P(SEQ, "head")
    return jax.shard_map(
        per_device, mesh=split, in_specs=in_specs, out_specs=out_specs, check_vma=False
    )
```

```python
import functools

import jax
import jax.numpy as jnp
import numpy as np
from jax import lax
from jax.experimental import pallas as pl
from jax.experimental.pallas import tpu as pltpu
from jax.sharding import Mesh
from jax.sharding import PartitionSpec as P


ROWS = 160
CHUNK = 256
SEQ = ("seq_0", "seq_1", "seq_2")
STEPS = (2, 1, 3)
MIB = 2**20
HEAD_LIMIT, OUT_LIMIT = (48 * MIB, 20 * MIB)
SLOTS = (0, 2, 1, 3)
OUT_STEPS = (0, 2, 1, 3)
GROUPS = ((0,), (2, 1), (3,))
FETCH_STEP = 2
F32, BF16 = (jnp.float32, jnp.bfloat16)
VMEM = pl.BlockSpec(memory_space=pltpu.VMEM)
SMEM = pl.BlockSpec(memory_space=pltpu.SMEM)
ANY = pl.BlockSpec(memory_space=pl.ANY)
NN = (((1,), (0,)), ((), ()))


def mm(a, b):
    return lax.dot_general(a, b, NN, preferred_element_type=F32)


def quarter_of(step):
    return lax.axis_index(SEQ[2]) ^ step


def feature_tables():
    first, second, scale = ([-1] * ROWS, [-1] * ROWS, [0.0] * ROWS)
    for d in range(9):
        for a in range(16 if d < 8 else 8):
            row = 16 * d + a
            first[row], second[row] = (a, (a + d) % 16)
            scale[row] = 1.0 / 32.0 if d == 0 else 1.0 / 16.0
    for a in range(16):
        first[136 + a], scale[136 + a] = (a, 0.25)
    scale[152] = 1.0
    table = np.zeros((8, ROWS), np.float32)
    table[0], table[1], table[2] = (first, second, scale)
    table[3, 152] = 1.0
    table[4, 136:153] = scale[136:153]
    return table


def key_features(u):
    tok = u.shape[1]
    blocks = [u * u]
    for d in range(1, 9):
        blocks.append(u * pltpu.roll(u, 16 - d, 0))
    blocks[8] = blocks[8][:8]
    row = lax.broadcasted_iota(jnp.int32, (8, tok), 0)
    tail = jnp.where(row == 0, 1.0, 0.0)
    return jnp.concatenate(blocks + [u, tail], axis=0).astype(BF16)


def norm_rows(norm):
    top = jnp.transpose(norm[:128])[:1]
    rest = jnp.concatenate([norm[128:], jnp.zeros((96, 128), F32)], axis=0)
    low = jnp.transpose(rest)[:1]
    row = lax.broadcasted_iota(jnp.int32, (8, 128), 0)
    return jnp.where(row == 1, top, jnp.where(row == 2, low, 0.0))


def head_kernel(
    x_hbm, wk_hbm, wq_hbm, wv_hbm,
    q_out, kt_out, val_out, local_out, s0, s1, s2, s3,
    x, wkq, wv, acc, kt, x_sem, w_sem, v_sem,
):
    tok, width = x.shape
    cuts = 4
    cut = width // cuts
    kd = wk_hbm.shape[1]

    def wcopy(j, src, half):
        rows = pl.ds(j * cut, cut)
        return pltpu.make_async_copy(
            src.at[rows], wkq.at[half, rows], w_sem.at[2 * j + half]
        )

    def xcopy(j):
        cols = pl.ds(j * cut, cut)
        return pltpu.make_async_copy(x_hbm.at[:, cols], x.at[:, cols], x_sem.at[j])

    def vcopy(s):
        start = pl.multiple_of(quarter_of(SLOTS[s]) * 256, 256)
        return pltpu.make_async_copy(
            wv_hbm.at[:, pl.ds(start, 256)],
            wv.at[s // 2, :, pl.ds(s % 2 * 256, 256)],
            v_sem.at[s],
        )

    for j in range(cuts):
        wcopy(j, wk_hbm, 0).start()
        wcopy(j, wq_hbm, 1).start()
        xcopy(j).start()
    for j in range(cuts):
        wcopy(j, wk_hbm, 0).wait()
        wcopy(j, wq_hbm, 1).wait()
        xcopy(j).wait()
        vcopy(j).start()
        cols = slice(j * cut, (j + 1) * cut)
        both = jnp.concatenate([wkq[0, cols], wkq[1, cols]], axis=1)
        for rows in (slice(0, tok // 2), slice(tok // 2, tok)):
            part = mm(x[rows, cols], both)
            acc[rows] = part if j == 0 else acc[rows] + part
    q_out[...] = acc[:, kd:].astype(BF16)
    keys = jnp.transpose(acc[:, :kd].astype(BF16).astype(F32))
    kt[...] = keys
    kt_out[...] = keys.astype(BF16)
    ones = jnp.ones((CHUNK, 128), BF16)
    for s, state in enumerate((s0, s1, s2, s3)):
        if s % 2 == 0:
            vcopy(s).wait()
            vcopy(s + 1).wait()
            pair = mm(x[...], wv[s // 2]).astype(BF16)
        val = pair[:, s % 2 * 256 : s % 2 * 256 + 256]
        val_out[s] = val
        for h in range(2):
            at = pl.multiple_of((quarter_of(SLOTS[s]) * 2 + h) * 16, 16)
            feat = key_features(kt[pl.ds(at, 16), :])
            run = None
            for c in range(tok // CHUNK):
                rows = slice(c * CHUNK, (c + 1) * CHUNK)
                right = jnp.concatenate([val[rows, h * 128 : (h + 1) * 128], ones], axis=1)
                part = mm(feat[:, rows], right)
                run = part if c == 0 else run + part
                if c < tok // CHUNK - 1:
                    local_out[s, h, c] = run.astype(BF16)
            state[h, :152] = run[:152, :128].astype(BF16)
            extra = norm_rows(run[:, 128:])
            row = lax.broadcasted_iota(jnp.int32, (8, 128), 0)
            state[h, 152:] = jnp.where(row == 0, run[152:, :128], extra).astype(BF16)


def head_stage(tokens, w_key, w_query, w_value):
    tok, width = tokens.shape
    kd = w_key.shape[1]
    chunks = tok // CHUNK
    shape = jax.ShapeDtypeStruct
    return pl.pallas_call(
        head_kernel,
        out_shape=[
            shape((tok, kd), BF16),
            shape((kd, tok), BF16),
            shape((4, tok, 256), BF16),
            shape((4, 2, chunks - 1, ROWS, 256), BF16),
        ]
        + [shape((2, ROWS, 128), BF16)] * 4,
        in_specs=[ANY] * 4,
        out_specs=[VMEM] * 8,
        scratch_shapes=[
            pltpu.VMEM((tok, width), BF16),
            pltpu.VMEM((2, width, kd), BF16),
            pltpu.VMEM((2, width, 512), BF16),
            pltpu.VMEM((tok, 2 * kd), F32),
            pltpu.VMEM((kd, tok), F32),
            pltpu.SemaphoreType.DMA((4,)),
            pltpu.SemaphoreType.DMA((8,)),
            pltpu.SemaphoreType.DMA((4,)),
        ],
        compiler_params=pltpu.CompilerParams(vmem_limit_bytes=HEAD_LIMIT),
        cost_estimate=pl.CostEstimate(
            flops=6 * 10**9, bytes_accessed=12 * 2**20, transcendentals=0
        ),
        name="head_stage",
    )(tokens, w_key, w_query, w_value)


def inner_kernel(slot, h, q_ref, kt_ref, val_ref, local_ref, table_ref, feat_out, part_out):
    tok = q_ref.shape[0]
    ones = jnp.ones((CHUNK, 128), BF16)
    below = lax.broadcasted_iota(jnp.int32, (CHUNK, CHUNK), 0) >= lax.broadcasted_iota(
        jnp.int32, (CHUNK, CHUNK), 1
    )
    first, second, scale = (table_ref[0:1], table_ref[1:2], table_ref[2:3])
    add_first, add_second = (table_ref[3:4], table_ref[4:5])
    entry = lax.broadcasted_iota(jnp.int32, (128, ROWS), 0).astype(F32)
    lane = lax.broadcasted_iota(jnp.int32, (CHUNK, 128), 1)
    at = (quarter_of(SLOTS[slot]) * 2 + h) * 16
    base = at.astype(F32)
    pick_first = jnp.where((entry == first + base) & (first >= 0), 1.0, 0.0).astype(BF16)
    pick_second = jnp.where((entry == second + base) & (second >= 0), scale, 0.0).astype(BF16)
    mine = (lane >= at) & (lane < at + 16)
    for c in range(tok // CHUNK):
        rows = slice(c * CHUNK, (c + 1) * CHUNK)
        q = q_ref[rows]
        feat = (mm(q, pick_first) + add_first) * (mm(q, pick_second) + add_second)
        feat = feat.astype(BF16)
        feat_out[rows] = feat
        own = jnp.where(mine, q.astype(F32) * 0.25, 0.0).astype(BF16)
        s = mm(own, kt_ref[:, rows])
        taylor = jnp.where(below, (0.5 * s + 1.0) * s + 1.0, 0.0).astype(BF16)
        right = jnp.concatenate([val_ref[slot, rows, h * 128 : (h + 1) * 128], ones], axis=1)
        part = mm(taylor, right)
        if c > 0:
            part = part + mm(feat, local_ref[slot, h, c - 1])
        part_out[rows] = part


def inner_stage(slot, h, *args):
    tok = args[0].shape[0]
    shape = jax.ShapeDtypeStruct
    return pl.pallas_call(
        functools.partial(inner_kernel, slot, h),
        out_shape=[shape((tok, ROWS), BF16), shape((tok, 256), F32)],
        in_specs=[VMEM] * 5,
        out_specs=[VMEM] * 2,
        compiler_params=pltpu.CompilerParams(vmem_limit_bytes=16 * MIB),
        cost_estimate=pl.CostEstimate(flops=10**9, bytes_accessed=2 * MIB, transcendentals=0),
        name="inner_stage",
    )(*args)


def outer_kernel(count, *refs):
    prefixes, (*inner, out) = (refs[:count], refs[count:])
    feats, parts = (inner[: 2 * count], inner[2 * count :])
    for i in range(count):
        for h in range(2):
            low = prefixes[i][h]
            wide = low[152:].astype(F32)
            top = jnp.transpose(jnp.broadcast_to(wide[1:2], (128, 128)))
            rest = jnp.transpose(jnp.broadcast_to(wide[2:3], (128, 128)))[:32]
            norm = jnp.concatenate([top, rest], axis=0).astype(BF16)
            right = jnp.concatenate([low, norm], axis=1)
            both = mm(feats[2 * i + h][...], right) + parts[2 * i + h][...]
            cols = slice(i * 256 + h * 128, i * 256 + (h + 1) * 128)
            out[:, cols] = (both[:, :128] / both[:, 128:]).astype(BF16)


def outer_stage(prefixes, feats, parts):
    count = len(prefixes)
    tok = feats[0].shape[0]
    return pl.pallas_call(
        functools.partial(outer_kernel, count),
        out_shape=jax.ShapeDtypeStruct((tok, 256 * count), BF16),
        in_specs=[VMEM] * (5 * count),
        out_specs=VMEM,
        compiler_params=pltpu.CompilerParams(vmem_limit_bytes=24 * 2**20),
        cost_estimate=pl.CostEstimate(
            flops=3 * 10**8 * count, bytes_accessed=2**20 * count, transcendentals=0
        ),
        name="outer_stage",
    )(*prefixes, *feats, *parts)


def fetch_copies(w_hbm, out, sem):
    own = lax.axis_index("head")
    cols = pl.ds(pl.multiple_of(own * 1024, 1024), 1024)
    copies = []
    for half in range(2):
        for s in range(4):
            row = (own ^ half) * 1024 + quarter_of(OUT_STEPS[s]) * 256
            source = w_hbm.at[pl.ds(pl.multiple_of(row, 256), 256), cols]
            target = out.at[half, pl.ds(s * 256, 256)]
            copies.append(pltpu.make_async_copy(source, target, sem.at[half * 4 + s]))
    return copies


def fetch_kernel(slot, q, kt, val, local, table, w_hbm, *rest):
    *outs, columns, sem = rest
    copies = fetch_copies(w_hbm, columns, sem)
    for copy in copies:
        copy.start()
    for h in range(2):
        inner_kernel(slot, h, q, kt, val, local, table, *outs[2 * h : 2 * h + 2])
    for copy in copies:
        copy.wait()


def fetch_stage(slot, *args):
    tok = args[0].shape[0]
    shape = jax.ShapeDtypeStruct
    *outs, columns = pl.pallas_call(
        functools.partial(fetch_kernel, slot),
        out_shape=[shape((tok, ROWS), BF16), shape((tok, 256), F32)] * 2
        + [shape((2, 1024, 1024), BF16)],
        in_specs=[VMEM] * 5 + [ANY],
        out_specs=[VMEM] * 5,
        scratch_shapes=[pltpu.SemaphoreType.DMA((8,))],
        compiler_params=pltpu.CompilerParams(vmem_limit_bytes=16 * MIB),
        cost_estimate=pl.CostEstimate(
            flops=2 * 10**9, bytes_accessed=4 * MIB, transcendentals=0
        ),
        name="fetch_stage",
    )(*args)
    return outs[:2], outs[2:], columns


def out_kernel(places, last, *refs):
    count = len(places)
    groups, (w_ref, *rest) = (refs[:count], refs[count:])
    tok = groups[0].shape[0]
    blocks = tok // CHUNK
    if last:
        acc, out, stage, sem = rest
        copies = []
        for c in range(blocks):
            rows = pl.ds(c * CHUNK, CHUNK)
            copies.append(pltpu.make_async_copy(stage.at[rows], out.at[rows], sem.at[c]))
    else:
        acc, out = (None, rest[0]) if len(rest) == 1 else rest
    for c in range(blocks):
        rows = slice(c * CHUNK, (c + 1) * CHUNK)
        part = None if acc is None else acc[rows]
        for group, (half, start, width) in zip(groups, places):
            more = mm(group[rows], w_ref[half, start : start + width])
            part = more if part is None else part + more
        if last:
            stage[rows] = part.astype(BF16)
            copies[c].start()
        else:
            out[rows] = part
    if last:
        for copy in copies:
            copy.wait()


def out_stage(groups, places, columns, acc=None, last=False):
    tok = groups[0].shape[0]
    args = [*groups, columns] + ([] if acc is None else [acc])
    depth = sum(width for _, _, width in places)
    return pl.pallas_call(
        functools.partial(out_kernel, places, last),
        out_shape=jax.ShapeDtypeStruct((tok, 1024), BF16 if last else F32),
        in_specs=[VMEM] * len(args),
        out_specs=ANY if last else VMEM,
        scratch_shapes=[pltpu.VMEM((tok, 1024), BF16), pltpu.SemaphoreType.DMA((tok // CHUNK,))]
        if last
        else [],
        compiler_params=pltpu.CompilerParams(vmem_limit_bytes=OUT_LIMIT),
        cost_estimate=pl.CostEstimate(
            flops=2 * tok * 1024 * depth, bytes_accessed=2**20, transcendentals=0
        ),
        name="out_stage",
    )(*args)


def partner(x, axis, step):
    pairs = [(i, i ^ step) for i in range(4)]
    return lax.ppermute(x, axis, pairs)


def total_kernel(p0, p1, p2, p3, out):
    total = p0[...].astype(F32) + p1[...].astype(F32)
    out[...] = (total + p2[...].astype(F32) + p3[...].astype(F32)).astype(BF16)


def level_kernel(axis, own, g0, g1, g2, base_in, total, base):
    at = lax.axis_index(axis)
    run, before = (own[...].astype(F32), jnp.zeros(own.shape, F32))
    if base_in is not None:
        before = base_in[...]
    for step, ref in zip(STEPS, (g0, g1, g2)):
        got = ref[...].astype(F32)
        run = run + got
        before = before + got * ((at ^ step) < at).astype(F32)
    if total is not None:
        total[...] = run.astype(BF16)
    base[...] = before


def spread_kernel(own, g0, g1, g2, base_in, p0, p1, p2, p3, o0, o1, o2, o3, base):
    level_kernel(SEQ[0], own, g0, g1, g2, base_in, None, base)
    at = lax.axis_index(SEQ[2])
    parts = [p[...].astype(F32) for p in (p0, p1, p2, p3)]
    for mine, out in zip(SLOTS, (o0, o1, o2, o3)):
        run = base[...]
        for step, part in zip(SLOTS, parts):
            run = run + part * ((at ^ step) < (at ^ mine)).astype(F32)
        out[...] = run.astype(BF16)


def small_call(kernel, outs, *args, scratch=(), after=()):
    shape = args[0].shape
    return pl.pallas_call(
        kernel,
        out_shape=[jax.ShapeDtypeStruct(shape, kind) for kind in outs],
        in_specs=[VMEM] * len(args) + [ANY] * len(after),
        out_specs=[VMEM] * len(outs),
        scratch_shapes=list(scratch),
        compiler_params=pltpu.CompilerParams(vmem_limit_bytes=4 * 2**20),
        cost_estimate=pl.CostEstimate(flops=10**6, bytes_accessed=2**20, transcendentals=0),
    )(*args, *after)


def middle_kernel(own, g0, g1, g2, columns, total, base):
    level_kernel(SEQ[1], own, g0, g1, g2, None, total, base)


def exclusive_prefix(states, columns):
    parts = [states[0]] + [partner(state, SEQ[2], step) for step, state in zip(STEPS, states[1:])]
    (low,) = small_call(total_kernel, [BF16], *parts)
    got = [partner(low, SEQ[1], step) for step in STEPS]
    total, base = small_call(middle_kernel, [BF16, F32], low, *got, after=[columns])
    got = [partner(total, SEQ[0], step) for step in STEPS]
    scratch = [pltpu.VMEM(low.shape, F32)]
    outs = small_call(spread_kernel, [BF16] * 4, total, *got, base, *parts, scratch=scratch)
    back = {0: outs[0]}
    for step, out in zip(STEPS, outs[1:]):
        back[step] = partner(out, SEQ[2], step)
    return back


def per_device(tokens, w_query, w_key, w_value, w_out):
    tokens, w_query, w_key, w_value, w_out = (
        pltpu.with_memory_space_constraint(x, pltpu.HBM)
        for x in (tokens, w_query, w_key, w_value, w_out)
    )
    table = jnp.asarray(feature_tables())
    q, kt, val, local, *states = head_stage(tokens, w_key, w_query, w_value)
    inner = {}
    args = (q, kt, val, local, table)
    for slot, step in enumerate(SLOTS):
        if step == FETCH_STEP:
            *pair, columns = fetch_stage(slot, *args, w_out)
            inner[step, 0], inner[step, 1] = pair
            continue
        for h in range(2):
            inner[step, h] = inner_stage(slot, h, *args)
    back = exclusive_prefix(states, columns)

    def outer(steps):
        return outer_stage(
            [back[step] for step in steps],
            [inner[step, h][0] for step in steps for h in range(2)],
            [inner[step, h][1] for step in steps for h in range(2)],
        )

    places, start = ([], 0)
    for steps in GROUPS:
        places.append((start, 256 * len(steps)))
        start += 256 * len(steps)
    own, other = ([], [])
    for steps in GROUPS:
        own.append(outer(steps))
        other.append(lax.ppermute(own[-1], "head", [(0, 1), (1, 0)]))
    mine = [(0, *place) for place in places]
    theirs = [(1, *place) for place in places]
    acc = out_stage(own[:1], mine[:1], columns)
    acc = out_stage([*own[1:], other[0]], (*mine[1:], theirs[0]), columns, acc)
    return out_stage(other[1:], theirs[1:], columns, acc, last=True)


def solution(mesh):
    split = Mesh(
        mesh.devices.reshape(4, 4, 4, mesh.shape["head"]), ("seq_0", "seq_1", "seq_2", "head")
    )
    in_specs = (P(SEQ, None), P(None, "head"), P(None, "head"), P(None, "head"), P())
    out_specs = P(SEQ, "head")
    return jax.shard_map(
        per_device, mesh=split, in_specs=in_specs, out_specs=out_specs, check_vma=False
    )
```

```python
import functools

import jax
import jax.numpy as jnp
import numpy as np
from jax import lax
from jax.experimental import pallas as pl
from jax.experimental.pallas import tpu as pltpu
from jax.sharding import Mesh
from jax.sharding import PartitionSpec as P


ROWS = 160
CHUNK = 256
SEQ = ("seq_0", "seq_1", "seq_2")
STEPS = (2, 1, 3)
MIB = 2**20
HEAD_LIMIT, OUT_LIMIT = (40 * MIB, 20 * MIB)
SLOTS = (0, 2, 1, 3)
OUT_STEPS = (0, 2, 1, 3)
GROUPS = ((0,), (2, 1), (3,))
F32, BF16 = (jnp.float32, jnp.bfloat16)
VMEM = pl.BlockSpec(memory_space=pltpu.VMEM)
SMEM = pl.BlockSpec(memory_space=pltpu.SMEM)
ANY = pl.BlockSpec(memory_space=pl.ANY)
NN = (((1,), (0,)), ((), ()))


def mm(a, b):
    return lax.dot_general(a, b, NN, preferred_element_type=F32)


def quarter_of(step):
    return lax.axis_index(SEQ[2]) ^ step


def feature_tables():
    first, second, scale = ([-1] * ROWS, [-1] * ROWS, [0.0] * ROWS)
    for d in range(9):
        for a in range(16 if d < 8 else 8):
            row = 16 * d + a
            first[row], second[row] = (a, (a + d) % 16)
            scale[row] = 1.0 / 32.0 if d == 0 else 1.0 / 16.0
    for a in range(16):
        first[136 + a], scale[136 + a] = (a, 0.25)
    scale[152] = 1.0
    table = np.zeros((8, ROWS), np.float32)
    table[0], table[1], table[2] = (first, second, scale)
    table[3, 152] = 1.0
    table[4, 136:153] = scale[136:153]
    return table


def key_features(u):
    tok = u.shape[1]
    blocks = [u * u]
    for d in range(1, 9):
        blocks.append(u * pltpu.roll(u, 16 - d, 0))
    blocks[8] = blocks[8][:8]
    row = lax.broadcasted_iota(jnp.int32, (8, tok), 0)
    tail = jnp.where(row == 0, 1.0, 0.0)
    return jnp.concatenate(blocks + [u, tail], axis=0).astype(BF16)


def norm_rows(norm):
    top = jnp.transpose(norm[:128])[:1]
    rest = jnp.concatenate([norm[128:], jnp.zeros((96, 128), F32)], axis=0)
    low = jnp.transpose(rest)[:1]
    row = lax.broadcasted_iota(jnp.int32, (8, 128), 0)
    return jnp.where(row == 1, top, jnp.where(row == 2, low, 0.0))


def fetch_copies(w_hbm, out, sem):
    own = lax.axis_index("head")
    cols = pl.ds(pl.multiple_of(own * 1024, 1024), 1024)
    copies = []
    for half in range(2):
        for s in range(4):
            row = (own ^ half) * 1024 + quarter_of(OUT_STEPS[s]) * 256
            source = w_hbm.at[pl.ds(pl.multiple_of(row, 256), 256), cols]
            target = out.at[half, pl.ds(s * 256, 256)]
            copies.append(pltpu.make_async_copy(source, target, sem.at[half * 4 + s]))
    return copies


def head_kernel(
    x_hbm, wk_hbm, wq_hbm, wv_hbm, out_hbm,
    q_out, kt_out, val_out, local_out, s0, s1, s2, s3, columns,
    x, wkq, wv, acc, kt, x_sem, w_sem, v_sem, c_sem,
):
    tok, width = x.shape
    cuts = 4
    cut = width // cuts
    kd = wk_hbm.shape[1]

    def wcopy(j, src, half):
        rows = pl.ds(j * cut, cut)
        return pltpu.make_async_copy(
            src.at[rows], wkq.at[half, rows], w_sem.at[2 * j + half]
        )

    def xcopy(j):
        cols = pl.ds(j * cut, cut)
        return pltpu.make_async_copy(x_hbm.at[:, cols], x.at[:, cols], x_sem.at[j])

    def vcopy(s):
        start = pl.multiple_of(quarter_of(SLOTS[s]) * 256, 256)
        return pltpu.make_async_copy(
            wv_hbm.at[:, pl.ds(start, 256)],
            wv.at[s // 2, :, pl.ds(s % 2 * 256, 256)],
            v_sem.at[s],
        )

    for j in range(cuts):
        wcopy(j, wk_hbm, 0).start()
        wcopy(j, wq_hbm, 1).start()
        xcopy(j).start()
    for j in range(cuts):
        wcopy(j, wk_hbm, 0).wait()
        wcopy(j, wq_hbm, 1).wait()
        xcopy(j).wait()
        vcopy(j).start()
        cols = slice(j * cut, (j + 1) * cut)
        both = jnp.concatenate([wkq[0, cols], wkq[1, cols]], axis=1)
        for rows in (slice(0, tok // 2), slice(tok // 2, tok)):
            part = mm(x[rows, cols], both)
            acc[rows] = part if j == 0 else acc[rows] + part
    fetches = fetch_copies(out_hbm, columns, c_sem)
    for fetch in fetches:
        fetch.start()
    q_out[...] = acc[:, kd:].astype(BF16)
    keys = jnp.transpose(acc[:, :kd].astype(BF16).astype(F32))
    kt[...] = keys
    kt_out[...] = keys.astype(BF16)
    ones = jnp.ones((CHUNK, 128), BF16)
    for s, state in enumerate((s0, s1, s2, s3)):
        if s % 2 == 0:
            vcopy(s).wait()
            vcopy(s + 1).wait()
            pair = mm(x[...], wv[s // 2]).astype(BF16)
        val = pair[:, s % 2 * 256 : s % 2 * 256 + 256]
        val_out[s] = val
        for h in range(2):
            at = pl.multiple_of((quarter_of(SLOTS[s]) * 2 + h) * 16, 16)
            feat = key_features(kt[pl.ds(at, 16), :])
            run = None
            for c in range(tok // CHUNK):
                rows = slice(c * CHUNK, (c + 1) * CHUNK)
                right = jnp.concatenate([val[rows, h * 128 : (h + 1) * 128], ones], axis=1)
                part = mm(feat[:, rows], right)
                run = part if c == 0 else run + part
                if c < tok // CHUNK - 1:
                    local_out[s, h, c] = run.astype(BF16)
            state[h, :152] = run[:152, :128].astype(BF16)
            extra = norm_rows(run[:, 128:])
            row = lax.broadcasted_iota(jnp.int32, (8, 128), 0)
            state[h, 152:] = jnp.where(row == 0, run[152:, :128], extra).astype(BF16)
    for fetch in fetches:
        fetch.wait()


def head_stage(tokens, w_key, w_query, w_value, w_out):
    tok, width = tokens.shape
    kd = w_key.shape[1]
    chunks = tok // CHUNK
    shape = jax.ShapeDtypeStruct
    return pl.pallas_call(
        head_kernel,
        out_shape=[
            shape((tok, kd), BF16),
            shape((kd, tok), BF16),
            shape((4, tok, 256), BF16),
            shape((4, 2, chunks - 1, ROWS, 256), BF16),
        ]
        + [shape((2, ROWS, 128), BF16)] * 4
        + [shape((2, 1024, 1024), BF16)],
        in_specs=[ANY] * 5,
        out_specs=[VMEM] * 9,
        scratch_shapes=[
            pltpu.VMEM((tok, width), BF16),
            pltpu.VMEM((2, width, kd), BF16),
            pltpu.VMEM((2, width, 512), BF16),
            pltpu.VMEM((tok, 2 * kd), F32),
            pltpu.VMEM((kd, tok), F32),
            pltpu.SemaphoreType.DMA((4,)),
            pltpu.SemaphoreType.DMA((8,)),
            pltpu.SemaphoreType.DMA((4,)),
            pltpu.SemaphoreType.DMA((8,)),
        ],
        compiler_params=pltpu.CompilerParams(vmem_limit_bytes=HEAD_LIMIT),
        cost_estimate=pl.CostEstimate(
            flops=6 * 10**9, bytes_accessed=12 * 2**20, transcendentals=0
        ),
        name="head_stage",
    )(tokens, w_key, w_query, w_value, w_out)


def inner_kernel(slot, h, q_ref, kt_ref, val_ref, local_ref, table_ref, feat_out, part_out):
    tok = q_ref.shape[0]
    ones = jnp.ones((CHUNK, 128), BF16)
    below = lax.broadcasted_iota(jnp.int32, (CHUNK, CHUNK), 0) >= lax.broadcasted_iota(
        jnp.int32, (CHUNK, CHUNK), 1
    )
    first, second, scale = (table_ref[0:1], table_ref[1:2], table_ref[2:3])
    add_first, add_second = (table_ref[3:4], table_ref[4:5])
    entry = lax.broadcasted_iota(jnp.int32, (128, ROWS), 0).astype(F32)
    lane = lax.broadcasted_iota(jnp.int32, (CHUNK, 128), 1)
    at = (quarter_of(SLOTS[slot]) * 2 + h) * 16
    base = at.astype(F32)
    pick_first = jnp.where((entry == first + base) & (first >= 0), 1.0, 0.0).astype(BF16)
    pick_second = jnp.where((entry == second + base) & (second >= 0), scale, 0.0).astype(BF16)
    mine = (lane >= at) & (lane < at + 16)
    for c in range(tok // CHUNK):
        rows = slice(c * CHUNK, (c + 1) * CHUNK)
        q = q_ref[rows]
        feat = (mm(q, pick_first) + add_first) * (mm(q, pick_second) + add_second)
        feat = feat.astype(BF16)
        feat_out[rows] = feat
        own = jnp.where(mine, q.astype(F32) * 0.25, 0.0).astype(BF16)
        s = mm(own, kt_ref[:, rows])
        taylor = jnp.where(below, (0.5 * s + 1.0) * s + 1.0, 0.0).astype(BF16)
        right = jnp.concatenate([val_ref[slot, rows, h * 128 : (h + 1) * 128], ones], axis=1)
        part = mm(taylor, right)
        if c > 0:
            part = part + mm(feat, local_ref[slot, h, c - 1])
        part_out[rows] = part


def inner_stage(slot, h, *args):
    tok = args[0].shape[0]
    shape = jax.ShapeDtypeStruct
    return pl.pallas_call(
        functools.partial(inner_kernel, slot, h),
        out_shape=[shape((tok, ROWS), BF16), shape((tok, 256), F32)],
        in_specs=[VMEM] * 5,
        out_specs=[VMEM] * 2,
        compiler_params=pltpu.CompilerParams(vmem_limit_bytes=16 * MIB),
        cost_estimate=pl.CostEstimate(flops=10**9, bytes_accessed=2 * MIB, transcendentals=0),
        name="inner_stage",
    )(*args)


def outer_kernel(count, *refs):
    prefixes, (*inner, out) = (refs[:count], refs[count:])
    feats, parts = (inner[: 2 * count], inner[2 * count :])
    for i in range(count):
        for h in range(2):
            low = prefixes[i][h]
            wide = low[152:].astype(F32)
            top = jnp.transpose(jnp.broadcast_to(wide[1:2], (128, 128)))
            rest = jnp.transpose(jnp.broadcast_to(wide[2:3], (128, 128)))[:32]
            norm = jnp.concatenate([top, rest], axis=0).astype(BF16)
            right = jnp.concatenate([low, norm], axis=1)
            both = mm(feats[2 * i + h][...], right) + parts[2 * i + h][...]
            cols = slice(i * 256 + h * 128, i * 256 + (h + 1) * 128)
            out[:, cols] = (both[:, :128] / both[:, 128:]).astype(BF16)


def outer_stage(prefixes, feats, parts):
    count = len(prefixes)
    tok = feats[0].shape[0]
    return pl.pallas_call(
        functools.partial(outer_kernel, count),
        out_shape=jax.ShapeDtypeStruct((tok, 256 * count), BF16),
        in_specs=[VMEM] * (5 * count),
        out_specs=VMEM,
        compiler_params=pltpu.CompilerParams(vmem_limit_bytes=24 * 2**20),
        cost_estimate=pl.CostEstimate(
            flops=3 * 10**8 * count, bytes_accessed=2**20 * count, transcendentals=0
        ),
        name="outer_stage",
    )(*prefixes, *feats, *parts)


def out_kernel(places, last, *refs):
    count = len(places)
    groups, (w_ref, *rest) = (refs[:count], refs[count:])
    tok = groups[0].shape[0]
    blocks = tok // CHUNK
    if last:
        acc, out, stage, sem = rest
        copies = []
        for c in range(blocks):
            rows = pl.ds(c * CHUNK, CHUNK)
            copies.append(pltpu.make_async_copy(stage.at[rows], out.at[rows], sem.at[c]))
    else:
        acc, out = (None, rest[0]) if len(rest) == 1 else rest
    for c in range(blocks):
        rows = slice(c * CHUNK, (c + 1) * CHUNK)
        part = None if acc is None else acc[rows]
        for group, (half, start, width) in zip(groups, places):
            more = mm(group[rows], w_ref[half, start : start + width])
            part = more if part is None else part + more
        if last:
            stage[rows] = part.astype(BF16)
            copies[c].start()
        else:
            out[rows] = part
    if last:
        for copy in copies:
            copy.wait()


def out_stage(groups, places, columns, acc=None, last=False):
    tok = groups[0].shape[0]
    args = [*groups, columns] + ([] if acc is None else [acc])
    depth = sum(width for _, _, width in places)
    return pl.pallas_call(
        functools.partial(out_kernel, places, last),
        out_shape=jax.ShapeDtypeStruct((tok, 1024), BF16 if last else F32),
        in_specs=[VMEM] * len(args),
        out_specs=ANY if last else VMEM,
        scratch_shapes=[pltpu.VMEM((tok, 1024), BF16), pltpu.SemaphoreType.DMA((tok // CHUNK,))]
        if last
        else [],
        compiler_params=pltpu.CompilerParams(vmem_limit_bytes=OUT_LIMIT),
        cost_estimate=pl.CostEstimate(
            flops=2 * tok * 1024 * depth, bytes_accessed=2**20, transcendentals=0
        ),
        name="out_stage",
    )(*args)


def partner(x, axis, step):
    pairs = [(i, i ^ step) for i in range(4)]
    return lax.ppermute(x, axis, pairs)


def total_kernel(p0, p1, p2, p3, out):
    total = p0[...].astype(F32) + p1[...].astype(F32)
    out[...] = (total + p2[...].astype(F32) + p3[...].astype(F32)).astype(BF16)


def level_kernel(axis, own, g0, g1, g2, base_in, total, base):
    at = lax.axis_index(axis)
    run, before = (own[...].astype(F32), jnp.zeros(own.shape, F32))
    if base_in is not None:
        before = base_in[...]
    for step, ref in zip(STEPS, (g0, g1, g2)):
        got = ref[...].astype(F32)
        run = run + got
        before = before + got * ((at ^ step) < at).astype(F32)
    if total is not None:
        total[...] = run.astype(BF16)
    base[...] = before


def spread_kernel(own, g0, g1, g2, base_in, p0, p1, p2, p3, o0, o1, o2, o3, base):
    level_kernel(SEQ[0], own, g0, g1, g2, base_in, None, base)
    at = lax.axis_index(SEQ[2])
    parts = [p[...].astype(F32) for p in (p0, p1, p2, p3)]
    for mine, out in zip(SLOTS, (o0, o1, o2, o3)):
        run = base[...]
        for step, part in zip(SLOTS, parts):
            run = run + part * ((at ^ step) < (at ^ mine)).astype(F32)
        out[...] = run.astype(BF16)


def small_call(kernel, outs, *args, scratch=()):
    shape = args[0].shape
    return pl.pallas_call(
        kernel,
        out_shape=[jax.ShapeDtypeStruct(shape, kind) for kind in outs],
        in_specs=[VMEM] * len(args),
        out_specs=[VMEM] * len(outs),
        scratch_shapes=list(scratch),
        compiler_params=pltpu.CompilerParams(vmem_limit_bytes=4 * 2**20),
        cost_estimate=pl.CostEstimate(flops=10**6, bytes_accessed=2**20, transcendentals=0),
    )(*args)


def middle_kernel(own, g0, g1, g2, total, base):
    level_kernel(SEQ[1], own, g0, g1, g2, None, total, base)


def exclusive_prefix(states):
    parts = [states[0]] + [partner(state, SEQ[2], step) for step, state in zip(STEPS, states[1:])]
    (low,) = small_call(total_kernel, [BF16], *parts)
    got = [partner(low, SEQ[1], step) for step in STEPS]
    total, base = small_call(middle_kernel, [BF16, F32], low, *got)
    got = [partner(total, SEQ[0], step) for step in STEPS]
    scratch = [pltpu.VMEM(low.shape, F32)]
    outs = small_call(spread_kernel, [BF16] * 4, total, *got, base, *parts, scratch=scratch)
    back = {0: outs[0]}
    for step, out in zip(STEPS, outs[1:]):
        back[step] = partner(out, SEQ[2], step)
    return back


def per_device(tokens, w_query, w_key, w_value, w_out):
    tokens, w_query, w_key, w_value, w_out = (
        pltpu.with_memory_space_constraint(x, pltpu.HBM)
        for x in (tokens, w_query, w_key, w_value, w_out)
    )
    table = jnp.asarray(feature_tables())
    q, kt, val, local, *states, columns = head_stage(
        tokens, w_key, w_query, w_value, w_out
    )
    inner = {}
    args = (q, kt, val, local, table)
    for slot, step in enumerate(SLOTS):
        for h in range(2):
            inner[step, h] = inner_stage(slot, h, *args)
    back = exclusive_prefix(states)

    def outer(steps):
        return outer_stage(
            [back[step] for step in steps],
            [inner[step, h][0] for step in steps for h in range(2)],
            [inner[step, h][1] for step in steps for h in range(2)],
        )

    places, start = ([], 0)
    for steps in GROUPS:
        places.append((start, 256 * len(steps)))
        start += 256 * len(steps)
    own, other = ([], [])
    for steps in GROUPS:
        own.append(outer(steps))
        other.append(lax.ppermute(own[-1], "head", [(0, 1), (1, 0)]))
    mine = [(0, *place) for place in places]
    theirs = [(1, *place) for place in places]
    acc = out_stage(own[:1], mine[:1], columns)
    acc = out_stage([*own[1:], other[0]], (*mine[1:], theirs[0]), columns, acc)
    return out_stage(other[1:], theirs[1:], columns, acc, last=True)


def solution(mesh):
    split = Mesh(
        mesh.devices.reshape(4, 4, 4, mesh.shape["head"]), ("seq_0", "seq_1", "seq_2", "head")
    )
    in_specs = (P(SEQ, None), P(None, "head"), P(None, "head"), P(None, "head"), P())
    out_specs = P(SEQ, "head")
    return jax.shard_map(
        per_device, mesh=split, in_specs=in_specs, out_specs=out_specs, check_vma=False
    )
```

```python
import functools

import jax
import jax.numpy as jnp
import numpy as np
from jax import lax
from jax.experimental import pallas as pl
from jax.experimental.pallas import tpu as pltpu
from jax.sharding import Mesh
from jax.sharding import PartitionSpec as P


ROWS = 160
CHUNK = 256
SEQ = ("seq_0", "seq_1", "seq_2")
STEPS = (1, 3, 2)
MIB = 2**20
HEAD_LIMIT, OUT_LIMIT = (40 * MIB, 20 * MIB)
SLOTS = (0, 1, 3, 2)
OUT_STEPS = (0, 1, 3, 2)
GROUPS = ((0,), (1, 3), (2,))
F32, BF16 = (jnp.float32, jnp.bfloat16)
VMEM = pl.BlockSpec(memory_space=pltpu.VMEM)
SMEM = pl.BlockSpec(memory_space=pltpu.SMEM)
ANY = pl.BlockSpec(memory_space=pl.ANY)
NN = (((1,), (0,)), ((), ()))


def mm(a, b):
    return lax.dot_general(a, b, NN, preferred_element_type=F32)


def quarter_of(step):
    return lax.axis_index(SEQ[2]) ^ step


def feature_tables():
    first, second, scale = ([-1] * ROWS, [-1] * ROWS, [0.0] * ROWS)
    for d in range(9):
        for a in range(16 if d < 8 else 8):
            row = 16 * d + a
            first[row], second[row] = (a, (a + d) % 16)
            scale[row] = 1.0 / 32.0 if d == 0 else 1.0 / 16.0
    for a in range(16):
        first[136 + a], scale[136 + a] = (a, 0.25)
    scale[152] = 1.0
    table = np.zeros((8, ROWS), np.float32)
    table[0], table[1], table[2] = (first, second, scale)
    table[3, 152] = 1.0
    table[4, 136:153] = scale[136:153]
    return table


def key_features(u):
    tok = u.shape[1]
    blocks = [u * u]
    for d in range(1, 9):
        blocks.append(u * pltpu.roll(u, 16 - d, 0))
    blocks[8] = blocks[8][:8]
    row = lax.broadcasted_iota(jnp.int32, (8, tok), 0)
    tail = jnp.where(row == 0, 1.0, 0.0)
    return jnp.concatenate(blocks + [u, tail], axis=0).astype(BF16)


def norm_rows(norm):
    top = jnp.transpose(norm[:128])[:1]
    rest = jnp.concatenate([norm[128:], jnp.zeros((96, 128), F32)], axis=0)
    low = jnp.transpose(rest)[:1]
    row = lax.broadcasted_iota(jnp.int32, (8, 128), 0)
    return jnp.where(row == 1, top, jnp.where(row == 2, low, 0.0))


def fetch_copies(w_hbm, out, sem):
    own = lax.axis_index("head")
    cols = pl.ds(pl.multiple_of(own * 1024, 1024), 1024)
    copies = []
    for half in range(2):
        for s in range(4):
            row = (own ^ half) * 1024 + quarter_of(OUT_STEPS[s]) * 256
            source = w_hbm.at[pl.ds(pl.multiple_of(row, 256), 256), cols]
            target = out.at[half, pl.ds(s * 256, 256)]
            copies.append(pltpu.make_async_copy(source, target, sem.at[half * 4 + s]))
    return copies


def head_kernel(
    x_hbm, wk_hbm, wq_hbm, wv_hbm, out_hbm,
    q_out, kt_out, val_out, local_out, s0, s1, s2, s3, columns,
    x, wkq, wv, acc, kt, x_sem, w_sem, v_sem, c_sem,
):
    tok, width = x.shape
    cuts = 4
    cut = width // cuts
    kd = wk_hbm.shape[1]

    def wcopy(j, src, half):
        rows = pl.ds(j * cut, cut)
        return pltpu.make_async_copy(
            src.at[rows], wkq.at[half, rows], w_sem.at[2 * j + half]
        )

    def xcopy(j):
        cols = pl.ds(j * cut, cut)
        return pltpu.make_async_copy(x_hbm.at[:, cols], x.at[:, cols], x_sem.at[j])

    def vcopy(s):
        start = pl.multiple_of(quarter_of(SLOTS[s]) * 256, 256)
        return pltpu.make_async_copy(
            wv_hbm.at[:, pl.ds(start, 256)],
            wv.at[s // 2, :, pl.ds(s % 2 * 256, 256)],
            v_sem.at[s],
        )

    for j in range(cuts):
        wcopy(j, wk_hbm, 0).start()
        wcopy(j, wq_hbm, 1).start()
        xcopy(j).start()
    for j in range(cuts):
        wcopy(j, wk_hbm, 0).wait()
        wcopy(j, wq_hbm, 1).wait()
        xcopy(j).wait()
        vcopy(j).start()
        cols = slice(j * cut, (j + 1) * cut)
        both = jnp.concatenate([wkq[0, cols], wkq[1, cols]], axis=1)
        for rows in (slice(0, tok // 2), slice(tok // 2, tok)):
            part = mm(x[rows, cols], both)
            acc[rows] = part if j == 0 else acc[rows] + part
    fetches = fetch_copies(out_hbm, columns, c_sem)
    for fetch in fetches:
        fetch.start()
    q_out[...] = acc[:, kd:].astype(BF16)
    keys = jnp.transpose(acc[:, :kd].astype(BF16).astype(F32))
    kt[...] = keys
    kt_out[...] = keys.astype(BF16)
    ones = jnp.ones((CHUNK, 128), BF16)
    for s, state in enumerate((s0, s1, s2, s3)):
        if s % 2 == 0:
            vcopy(s).wait()
            vcopy(s + 1).wait()
            pair = mm(x[...], wv[s // 2]).astype(BF16)
        val = pair[:, s % 2 * 256 : s % 2 * 256 + 256]
        val_out[s] = val
        for h in range(2):
            at = pl.multiple_of((quarter_of(SLOTS[s]) * 2 + h) * 16, 16)
            feat = key_features(kt[pl.ds(at, 16), :])
            run = None
            for c in range(tok // CHUNK):
                rows = slice(c * CHUNK, (c + 1) * CHUNK)
                right = jnp.concatenate([val[rows, h * 128 : (h + 1) * 128], ones], axis=1)
                part = mm(feat[:, rows], right)
                run = part if c == 0 else run + part
                if c < tok // CHUNK - 1:
                    local_out[s, h, c] = run.astype(BF16)
            state[h, :152] = run[:152, :128].astype(BF16)
            extra = norm_rows(run[:, 128:])
            row = lax.broadcasted_iota(jnp.int32, (8, 128), 0)
            state[h, 152:] = jnp.where(row == 0, run[152:, :128], extra).astype(BF16)
    for fetch in fetches:
        fetch.wait()


def head_stage(tokens, w_key, w_query, w_value, w_out):
    tok, width = tokens.shape
    kd = w_key.shape[1]
    chunks = tok // CHUNK
    shape = jax.ShapeDtypeStruct
    return pl.pallas_call(
        head_kernel,
        out_shape=[
            shape((tok, kd), BF16),
            shape((kd, tok), BF16),
            shape((4, tok, 256), BF16),
            shape((4, 2, chunks - 1, ROWS, 256), BF16),
        ]
        + [shape((2, ROWS, 128), BF16)] * 4
        + [shape((2, 1024, 1024), BF16)],
        in_specs=[ANY] * 5,
        out_specs=[VMEM] * 9,
        scratch_shapes=[
            pltpu.VMEM((tok, width), BF16),
            pltpu.VMEM((2, width, kd), BF16),
            pltpu.VMEM((2, width, 512), BF16),
            pltpu.VMEM((tok, 2 * kd), F32),
            pltpu.VMEM((kd, tok), F32),
            pltpu.SemaphoreType.DMA((4,)),
            pltpu.SemaphoreType.DMA((8,)),
            pltpu.SemaphoreType.DMA((4,)),
            pltpu.SemaphoreType.DMA((8,)),
        ],
        compiler_params=pltpu.CompilerParams(vmem_limit_bytes=HEAD_LIMIT),
        cost_estimate=pl.CostEstimate(
            flops=6 * 10**9, bytes_accessed=12 * 2**20, transcendentals=0
        ),
        name="head_stage",
    )(tokens, w_key, w_query, w_value, w_out)


def inner_kernel(slot, h, q_ref, kt_ref, val_ref, local_ref, table_ref, feat_out, part_out):
    tok = q_ref.shape[0]
    ones = jnp.ones((CHUNK, 128), BF16)
    below = lax.broadcasted_iota(jnp.int32, (CHUNK, CHUNK), 0) >= lax.broadcasted_iota(
        jnp.int32, (CHUNK, CHUNK), 1
    )
    first, second, scale = (table_ref[0:1], table_ref[1:2], table_ref[2:3])
    add_first, add_second = (table_ref[3:4], table_ref[4:5])
    entry = lax.broadcasted_iota(jnp.int32, (128, ROWS), 0).astype(F32)
    lane = lax.broadcasted_iota(jnp.int32, (CHUNK, 128), 1)
    at = (quarter_of(SLOTS[slot]) * 2 + h) * 16
    base = at.astype(F32)
    pick_first = jnp.where((entry == first + base) & (first >= 0), 1.0, 0.0).astype(BF16)
    pick_second = jnp.where((entry == second + base) & (second >= 0), scale, 0.0).astype(BF16)
    mine = (lane >= at) & (lane < at + 16)
    for c in range(tok // CHUNK):
        rows = slice(c * CHUNK, (c + 1) * CHUNK)
        q = q_ref[rows]
        feat = (mm(q, pick_first) + add_first) * (mm(q, pick_second) + add_second)
        feat = feat.astype(BF16)
        feat_out[rows] = feat
        own = jnp.where(mine, q.astype(F32) * 0.25, 0.0).astype(BF16)
        s = mm(own, kt_ref[:, rows])
        taylor = jnp.where(below, (0.5 * s + 1.0) * s + 1.0, 0.0).astype(BF16)
        right = jnp.concatenate([val_ref[slot, rows, h * 128 : (h + 1) * 128], ones], axis=1)
        part = mm(taylor, right)
        if c > 0:
            part = part + mm(feat, local_ref[slot, h, c - 1])
        part_out[rows] = part


def inner_stage(slot, h, *args):
    tok = args[0].shape[0]
    shape = jax.ShapeDtypeStruct
    return pl.pallas_call(
        functools.partial(inner_kernel, slot, h),
        out_shape=[shape((tok, ROWS), BF16), shape((tok, 256), F32)],
        in_specs=[VMEM] * 5,
        out_specs=[VMEM] * 2,
        compiler_params=pltpu.CompilerParams(vmem_limit_bytes=16 * MIB),
        cost_estimate=pl.CostEstimate(flops=10**9, bytes_accessed=2 * MIB, transcendentals=0),
        name="inner_stage",
    )(*args)


def outer_kernel(count, *refs):
    prefixes, (*inner, out) = (refs[:count], refs[count:])
    feats, parts = (inner[: 2 * count], inner[2 * count :])
    for i in range(count):
        for h in range(2):
            low = prefixes[i][h]
            wide = low[152:].astype(F32)
            top = jnp.transpose(jnp.broadcast_to(wide[1:2], (128, 128)))
            rest = jnp.transpose(jnp.broadcast_to(wide[2:3], (128, 128)))[:32]
            norm = jnp.concatenate([top, rest], axis=0).astype(BF16)
            right = jnp.concatenate([low, norm], axis=1)
            both = mm(feats[2 * i + h][...], right) + parts[2 * i + h][...]
            cols = slice(i * 256 + h * 128, i * 256 + (h + 1) * 128)
            out[:, cols] = (both[:, :128] / both[:, 128:]).astype(BF16)


def outer_stage(prefixes, feats, parts):
    count = len(prefixes)
    tok = feats[0].shape[0]
    return pl.pallas_call(
        functools.partial(outer_kernel, count),
        out_shape=jax.ShapeDtypeStruct((tok, 256 * count), BF16),
        in_specs=[VMEM] * (5 * count),
        out_specs=VMEM,
        compiler_params=pltpu.CompilerParams(vmem_limit_bytes=24 * 2**20),
        cost_estimate=pl.CostEstimate(
            flops=3 * 10**8 * count, bytes_accessed=2**20 * count, transcendentals=0
        ),
        name="outer_stage",
    )(*prefixes, *feats, *parts)


def out_kernel(places, last, *refs):
    count = len(places)
    groups, (w_ref, *rest) = (refs[:count], refs[count:])
    tok = groups[0].shape[0]
    blocks = tok // CHUNK
    if last:
        acc, out, stage, sem = rest
        copies = []
        for c in range(blocks):
            rows = pl.ds(c * CHUNK, CHUNK)
            copies.append(pltpu.make_async_copy(stage.at[rows], out.at[rows], sem.at[c]))
    else:
        acc, out = (None, rest[0]) if len(rest) == 1 else rest
    for c in range(blocks):
        rows = slice(c * CHUNK, (c + 1) * CHUNK)
        part = None if acc is None else acc[rows]
        for group, (half, start, width) in zip(groups, places):
            more = mm(group[rows], w_ref[half, start : start + width])
            part = more if part is None else part + more
        if last:
            stage[rows] = part.astype(BF16)
            copies[c].start()
        else:
            out[rows] = part
    if last:
        for copy in copies:
            copy.wait()


def out_stage(groups, places, columns, acc=None, last=False):
    tok = groups[0].shape[0]
    args = [*groups, columns] + ([] if acc is None else [acc])
    depth = sum(width for _, _, width in places)
    return pl.pallas_call(
        functools.partial(out_kernel, places, last),
        out_shape=jax.ShapeDtypeStruct((tok, 1024), BF16 if last else F32),
        in_specs=[VMEM] * len(args),
        out_specs=ANY if last else VMEM,
        scratch_shapes=[pltpu.VMEM((tok, 1024), BF16), pltpu.SemaphoreType.DMA((tok // CHUNK,))]
        if last
        else [],
        compiler_params=pltpu.CompilerParams(vmem_limit_bytes=OUT_LIMIT),
        cost_estimate=pl.CostEstimate(
            flops=2 * tok * 1024 * depth, bytes_accessed=2**20, transcendentals=0
        ),
        name="out_stage",
    )(*args)


def partner(x, axis, step):
    pairs = [(i, i ^ step) for i in range(4)]
    return lax.ppermute(x, axis, pairs)


def total_kernel(p0, p1, p2, p3, out):
    total = p0[...].astype(F32) + p1[...].astype(F32)
    out[...] = (total + p2[...].astype(F32) + p3[...].astype(F32)).astype(BF16)


def level_kernel(axis, own, g0, g1, g2, base_in, total, base):
    at = lax.axis_index(axis)
    run, before = (own[...].astype(F32), jnp.zeros(own.shape, F32))
    if base_in is not None:
        before = base_in[...]
    for step, ref in zip(STEPS, (g0, g1, g2)):
        got = ref[...].astype(F32)
        run = run + got
        before = before + got * ((at ^ step) < at).astype(F32)
    if total is not None:
        total[...] = run.astype(BF16)
    base[...] = before


def spread_kernel(own, g0, g1, g2, base_in, p0, p1, p2, p3, o0, o1, o2, o3, base):
    level_kernel(SEQ[0], own, g0, g1, g2, base_in, None, base)
    at = lax.axis_index(SEQ[2])
    parts = [p[...].astype(F32) for p in (p0, p1, p2, p3)]
    for mine, out in zip(SLOTS, (o0, o1, o2, o3)):
        run = base[...]
        for step, part in zip(SLOTS, parts):
            run = run + part * ((at ^ step) < (at ^ mine)).astype(F32)
        out[...] = run.astype(BF16)


def small_call(kernel, outs, *args, scratch=()):
    shape = args[0].shape
    return pl.pallas_call(
        kernel,
        out_shape=[jax.ShapeDtypeStruct(shape, kind) for kind in outs],
        in_specs=[VMEM] * len(args),
        out_specs=[VMEM] * len(outs),
        scratch_shapes=list(scratch),
        compiler_params=pltpu.CompilerParams(vmem_limit_bytes=4 * 2**20),
        cost_estimate=pl.CostEstimate(flops=10**6, bytes_accessed=2**20, transcendentals=0),
    )(*args)


def middle_kernel(own, g0, g1, g2, total, base):
    level_kernel(SEQ[1], own, g0, g1, g2, None, total, base)


def exclusive_prefix(states):
    parts = [states[0]] + [partner(state, SEQ[2], step) for step, state in zip(STEPS, states[1:])]
    (low,) = small_call(total_kernel, [BF16], *parts)
    got = [partner(low, SEQ[1], step) for step in STEPS]
    total, base = small_call(middle_kernel, [BF16, F32], low, *got)
    got = [partner(total, SEQ[0], step) for step in STEPS]
    scratch = [pltpu.VMEM(low.shape, F32)]
    outs = small_call(spread_kernel, [BF16] * 4, total, *got, base, *parts, scratch=scratch)
    back = {0: outs[0]}
    for step, out in zip(STEPS, outs[1:]):
        back[step] = partner(out, SEQ[2], step)
    return back


def per_device(tokens, w_query, w_key, w_value, w_out):
    tokens, w_query, w_key, w_value, w_out = (
        pltpu.with_memory_space_constraint(x, pltpu.HBM)
        for x in (tokens, w_query, w_key, w_value, w_out)
    )
    table = jnp.asarray(feature_tables())
    q, kt, val, local, *states, columns = head_stage(
        tokens, w_key, w_query, w_value, w_out
    )
    inner = {}
    args = (q, kt, val, local, table)
    for slot, step in enumerate(SLOTS):
        for h in range(2):
            inner[step, h] = inner_stage(slot, h, *args)
    back = exclusive_prefix(states)

    def outer(steps):
        return outer_stage(
            [back[step] for step in steps],
            [inner[step, h][0] for step in steps for h in range(2)],
            [inner[step, h][1] for step in steps for h in range(2)],
        )

    places, start = ([], 0)
    for steps in GROUPS:
        places.append((start, 256 * len(steps)))
        start += 256 * len(steps)
    own, other = ([], [])
    for steps in GROUPS:
        own.append(outer(steps))
        other.append(lax.ppermute(own[-1], "head", [(0, 1), (1, 0)]))
    mine = [(0, *place) for place in places]
    theirs = [(1, *place) for place in places]
    acc = out_stage(own[:1], mine[:1], columns)
    acc = out_stage([*own[1:], other[0]], (*mine[1:], theirs[0]), columns, acc)
    return out_stage(other[1:], theirs[1:], columns, acc, last=True)


def solution(mesh):
    split = Mesh(
        mesh.devices.reshape(4, 4, 4, mesh.shape["head"]), ("seq_0", "seq_1", "seq_2", "head")
    )
    in_specs = (P(SEQ, None), P(None, "head"), P(None, "head"), P(None, "head"), P())
    out_specs = P(SEQ, "head")
    return jax.shard_map(
        per_device, mesh=split, in_specs=in_specs, out_specs=out_specs, check_vma=False
    )
```

```python
import functools

import jax
import jax.numpy as jnp
import numpy as np
from jax import lax
from jax.experimental import pallas as pl
from jax.experimental.pallas import tpu as pltpu
from jax.sharding import Mesh
from jax.sharding import PartitionSpec as P


ROWS = 160
CHUNK = 256
SEQ = ("seq_0", "seq_1", "seq_2")
STEPS = (1, 2, 3)
MIB = 2**20
HEAD_LIMIT, OUT_LIMIT = (40 * MIB, 20 * MIB)
SLOTS = (0, 1, 2, 3)
OUT_STEPS = (0, 2, 1, 3)
GROUPS = ((0,), (2, 1), (3,))
F32, BF16 = (jnp.float32, jnp.bfloat16)
VMEM = pl.BlockSpec(memory_space=pltpu.VMEM)
SMEM = pl.BlockSpec(memory_space=pltpu.SMEM)
ANY = pl.BlockSpec(memory_space=pl.ANY)
NN = (((1,), (0,)), ((), ()))


def mm(a, b):
    return lax.dot_general(a, b, NN, preferred_element_type=F32)


def quarter_of(step):
    return lax.axis_index(SEQ[2]) ^ step


def feature_tables():
    first, second, scale = ([-1] * ROWS, [-1] * ROWS, [0.0] * ROWS)
    for d in range(9):
        for a in range(16 if d < 8 else 8):
            row = 16 * d + a
            first[row], second[row] = (a, (a + d) % 16)
            scale[row] = 1.0 / 32.0 if d == 0 else 1.0 / 16.0
    for a in range(16):
        first[136 + a], scale[136 + a] = (a, 0.25)
    scale[152] = 1.0
    table = np.zeros((8, ROWS), np.float32)
    table[0], table[1], table[2] = (first, second, scale)
    table[3, 152] = 1.0
    table[4, 136:153] = scale[136:153]
    return table


def key_features(u):
    tok = u.shape[1]
    blocks = [u * u]
    for d in range(1, 9):
        blocks.append(u * pltpu.roll(u, 16 - d, 0))
    blocks[8] = blocks[8][:8]
    row = lax.broadcasted_iota(jnp.int32, (8, tok), 0)
    tail = jnp.where(row == 0, 1.0, 0.0)
    return jnp.concatenate(blocks + [u, tail], axis=0).astype(BF16)


def norm_rows(norm):
    top = jnp.transpose(norm[:128])[:1]
    rest = jnp.concatenate([norm[128:], jnp.zeros((96, 128), F32)], axis=0)
    low = jnp.transpose(rest)[:1]
    row = lax.broadcasted_iota(jnp.int32, (8, 128), 0)
    return jnp.where(row == 1, top, jnp.where(row == 2, low, 0.0))


def fetch_copies(w_hbm, out, sem):
    own = lax.axis_index("head")
    cols = pl.ds(pl.multiple_of(own * 1024, 1024), 1024)
    copies = []
    for half in range(2):
        for s in range(4):
            row = (own ^ half) * 1024 + quarter_of(OUT_STEPS[s]) * 256
            source = w_hbm.at[pl.ds(pl.multiple_of(row, 256), 256), cols]
            target = out.at[half, pl.ds(s * 256, 256)]
            copies.append(pltpu.make_async_copy(source, target, sem.at[half * 4 + s]))
    return copies


def head_kernel(
    x_hbm, wk_hbm, wq_hbm, wv_hbm, out_hbm,
    q_out, kt_out, val_out, local_out, s0, s1, s2, s3, columns,
    x, wkq, wv, acc, kt, x_sem, w_sem, v_sem, c_sem,
):
    tok, width = x.shape
    cuts = 4
    cut = width // cuts
    kd = wk_hbm.shape[1]

    def wcopy(j, src, half):
        rows = pl.ds(j * cut, cut)
        return pltpu.make_async_copy(
            src.at[rows], wkq.at[half, rows], w_sem.at[2 * j + half]
        )

    def xcopy(j):
        cols = pl.ds(j * cut, cut)
        return pltpu.make_async_copy(x_hbm.at[:, cols], x.at[:, cols], x_sem.at[j])

    def vcopy(s):
        start = pl.multiple_of(quarter_of(SLOTS[s]) * 256, 256)
        return pltpu.make_async_copy(
            wv_hbm.at[:, pl.ds(start, 256)],
            wv.at[s // 2, :, pl.ds(s % 2 * 256, 256)],
            v_sem.at[s],
        )

    for j in range(cuts):
        wcopy(j, wk_hbm, 0).start()
        wcopy(j, wq_hbm, 1).start()
        xcopy(j).start()
    for j in range(cuts):
        wcopy(j, wk_hbm, 0).wait()
        wcopy(j, wq_hbm, 1).wait()
        xcopy(j).wait()
        vcopy(j).start()
        cols = slice(j * cut, (j + 1) * cut)
        both = jnp.concatenate([wkq[0, cols], wkq[1, cols]], axis=1)
        for rows in (slice(0, tok // 2), slice(tok // 2, tok)):
            part = mm(x[rows, cols], both)
            acc[rows] = part if j == 0 else acc[rows] + part
    fetches = fetch_copies(out_hbm, columns, c_sem)
    for fetch in fetches:
        fetch.start()
    q_out[...] = acc[:, kd:].astype(BF16)
    keys = jnp.transpose(acc[:, :kd].astype(BF16).astype(F32))
    kt[...] = keys
    kt_out[...] = keys.astype(BF16)
    ones = jnp.ones((CHUNK, 128), BF16)
    for s, state in enumerate((s0, s1, s2, s3)):
        if s % 2 == 0:
            vcopy(s).wait()
            vcopy(s + 1).wait()
            pair = mm(x[...], wv[s // 2]).astype(BF16)
        val = pair[:, s % 2 * 256 : s % 2 * 256 + 256]
        val_out[s] = val
        for h in range(2):
            at = pl.multiple_of((quarter_of(SLOTS[s]) * 2 + h) * 16, 16)
            feat = key_features(kt[pl.ds(at, 16), :])
            run = None
            for c in range(tok // CHUNK):
                rows = slice(c * CHUNK, (c + 1) * CHUNK)
                right = jnp.concatenate([val[rows, h * 128 : (h + 1) * 128], ones], axis=1)
                part = mm(feat[:, rows], right)
                run = part if c == 0 else run + part
                if c < tok // CHUNK - 1:
                    local_out[s, h, c] = run.astype(BF16)
            state[h, :152] = run[:152, :128].astype(BF16)
            extra = norm_rows(run[:, 128:])
            row = lax.broadcasted_iota(jnp.int32, (8, 128), 0)
            state[h, 152:] = jnp.where(row == 0, run[152:, :128], extra).astype(BF16)
    for fetch in fetches:
        fetch.wait()


def head_stage(tokens, w_key, w_query, w_value, w_out):
    tok, width = tokens.shape
    kd = w_key.shape[1]
    chunks = tok // CHUNK
    shape = jax.ShapeDtypeStruct
    return pl.pallas_call(
        head_kernel,
        out_shape=[
            shape((tok, kd), BF16),
            shape((kd, tok), BF16),
            shape((4, tok, 256), BF16),
            shape((4, 2, chunks - 1, ROWS, 256), BF16),
        ]
        + [shape((2, ROWS, 128), BF16)] * 4
        + [shape((2, 1024, 1024), BF16)],
        in_specs=[ANY] * 5,
        out_specs=[VMEM] * 9,
        scratch_shapes=[
            pltpu.VMEM((tok, width), BF16),
            pltpu.VMEM((2, width, kd), BF16),
            pltpu.VMEM((2, width, 512), BF16),
            pltpu.VMEM((tok, 2 * kd), F32),
            pltpu.VMEM((kd, tok), F32),
            pltpu.SemaphoreType.DMA((4,)),
            pltpu.SemaphoreType.DMA((8,)),
            pltpu.SemaphoreType.DMA((4,)),
            pltpu.SemaphoreType.DMA((8,)),
        ],
        compiler_params=pltpu.CompilerParams(vmem_limit_bytes=HEAD_LIMIT),
        cost_estimate=pl.CostEstimate(
            flops=6 * 10**9, bytes_accessed=12 * 2**20, transcendentals=0
        ),
        name="head_stage",
    )(tokens, w_key, w_query, w_value, w_out)


def inner_kernel(slot, h, q_ref, kt_ref, val_ref, local_ref, table_ref, feat_out, part_out):
    tok = q_ref.shape[0]
    ones = jnp.ones((CHUNK, 128), BF16)
    below = lax.broadcasted_iota(jnp.int32, (CHUNK, CHUNK), 0) >= lax.broadcasted_iota(
        jnp.int32, (CHUNK, CHUNK), 1
    )
    first, second, scale = (table_ref[0:1], table_ref[1:2], table_ref[2:3])
    add_first, add_second = (table_ref[3:4], table_ref[4:5])
    entry = lax.broadcasted_iota(jnp.int32, (128, ROWS), 0).astype(F32)
    lane = lax.broadcasted_iota(jnp.int32, (CHUNK, 128), 1)
    at = (quarter_of(SLOTS[slot]) * 2 + h) * 16
    base = at.astype(F32)
    pick_first = jnp.where((entry == first + base) & (first >= 0), 1.0, 0.0).astype(BF16)
    pick_second = jnp.where((entry == second + base) & (second >= 0), scale, 0.0).astype(BF16)
    mine = (lane >= at) & (lane < at + 16)
    for c in range(tok // CHUNK):
        rows = slice(c * CHUNK, (c + 1) * CHUNK)
        q = q_ref[rows]
        feat = (mm(q, pick_first) + add_first) * (mm(q, pick_second) + add_second)
        feat = feat.astype(BF16)
        feat_out[rows] = feat
        own = jnp.where(mine, q.astype(F32) * 0.25, 0.0).astype(BF16)
        s = mm(own, kt_ref[:, rows])
        taylor = jnp.where(below, (0.5 * s + 1.0) * s + 1.0, 0.0).astype(BF16)
        right = jnp.concatenate([val_ref[slot, rows, h * 128 : (h + 1) * 128], ones], axis=1)
        part = mm(taylor, right)
        if c > 0:
            part = part + mm(feat, local_ref[slot, h, c - 1])
        part_out[rows] = part


def inner_stage(slot, h, *args):
    tok = args[0].shape[0]
    shape = jax.ShapeDtypeStruct
    return pl.pallas_call(
        functools.partial(inner_kernel, slot, h),
        out_shape=[shape((tok, ROWS), BF16), shape((tok, 256), F32)],
        in_specs=[VMEM] * 5,
        out_specs=[VMEM] * 2,
        compiler_params=pltpu.CompilerParams(vmem_limit_bytes=16 * MIB),
        cost_estimate=pl.CostEstimate(flops=10**9, bytes_accessed=2 * MIB, transcendentals=0),
        name="inner_stage",
    )(*args)


def outer_kernel(count, *refs):
    prefixes, (*inner, out) = (refs[:count], refs[count:])
    feats, parts = (inner[: 2 * count], inner[2 * count :])
    for i in range(count):
        for h in range(2):
            low = prefixes[i][h]
            wide = low[152:].astype(F32)
            top = jnp.transpose(jnp.broadcast_to(wide[1:2], (128, 128)))
            rest = jnp.transpose(jnp.broadcast_to(wide[2:3], (128, 128)))[:32]
            norm = jnp.concatenate([top, rest], axis=0).astype(BF16)
            right = jnp.concatenate([low, norm], axis=1)
            cols = slice(i * 256 + h * 128, i * 256 + (h + 1) * 128)
            feat, part = (feats[2 * i + h], parts[2 * i + h])
            half = feat.shape[0] // 2
            for rows in (slice(0, half), slice(half, 2 * half)):
                both = mm(feat[rows], right) + part[rows]
                out[rows, cols] = (both[:, :128] / both[:, 128:]).astype(BF16)


def outer_stage(prefixes, feats, parts):
    count = len(prefixes)
    tok = feats[0].shape[0]
    return pl.pallas_call(
        functools.partial(outer_kernel, count),
        out_shape=jax.ShapeDtypeStruct((tok, 256 * count), BF16),
        in_specs=[VMEM] * (5 * count),
        out_specs=VMEM,
        compiler_params=pltpu.CompilerParams(vmem_limit_bytes=24 * 2**20),
        cost_estimate=pl.CostEstimate(
            flops=3 * 10**8 * count, bytes_accessed=2**20 * count, transcendentals=0
        ),
        name="outer_stage",
    )(*prefixes, *feats, *parts)


def out_kernel(places, last, *refs):
    count = len(places)
    groups, (w_ref, *rest) = (refs[:count], refs[count:])
    tok = groups[0].shape[0]
    blocks = tok // CHUNK
    if last:
        acc, out, stage, sem = rest
        copies = []
        for c in range(blocks):
            rows = pl.ds(c * CHUNK, CHUNK)
            copies.append(pltpu.make_async_copy(stage.at[rows], out.at[rows], sem.at[c]))
    else:
        acc, out = (None, rest[0]) if len(rest) == 1 else rest
    for c in range(blocks):
        rows = slice(c * CHUNK, (c + 1) * CHUNK)
        part = None if acc is None else acc[rows]
        for group, (half, start, width) in zip(groups, places):
            more = mm(group[rows], w_ref[half, start : start + width])
            part = more if part is None else part + more
        if last:
            stage[rows] = part.astype(BF16)
            copies[c].start()
        else:
            out[rows] = part
    if last:
        for copy in copies:
            copy.wait()


def out_stage(groups, places, columns, acc=None, last=False):
    tok = groups[0].shape[0]
    args = [*groups, columns] + ([] if acc is None else [acc])
    depth = sum(width for _, _, width in places)
    return pl.pallas_call(
        functools.partial(out_kernel, places, last),
        out_shape=jax.ShapeDtypeStruct((tok, 1024), BF16 if last else F32),
        in_specs=[VMEM] * len(args),
        out_specs=ANY if last else VMEM,
        scratch_shapes=[pltpu.VMEM((tok, 1024), BF16), pltpu.SemaphoreType.DMA((tok // CHUNK,))]
        if last
        else [],
        compiler_params=pltpu.CompilerParams(vmem_limit_bytes=OUT_LIMIT),
        cost_estimate=pl.CostEstimate(
            flops=2 * tok * 1024 * depth, bytes_accessed=2**20, transcendentals=0
        ),
        name="out_stage",
    )(*args)


def partner(x, axis, step):
    pairs = [(i, i ^ step) for i in range(4)]
    return lax.ppermute(x, axis, pairs)


def total_kernel(p0, p1, p2, p3, out):
    total = p0[...].astype(F32) + p1[...].astype(F32)
    out[...] = (total + p2[...].astype(F32) + p3[...].astype(F32)).astype(BF16)


def level_kernel(axis, own, g0, g1, g2, base_in, total, base):
    at = lax.axis_index(axis)
    run, before = (own[...].astype(F32), jnp.zeros(own.shape, F32))
    if base_in is not None:
        before = base_in[...]
    for step, ref in zip(STEPS, (g0, g1, g2)):
        got = ref[...].astype(F32)
        run = run + got
        before = before + got * ((at ^ step) < at).astype(F32)
    if total is not None:
        total[...] = run.astype(BF16)
    base[...] = before


def spread_kernel(own, g0, g1, g2, base_in, p0, p1, p2, p3, o0, o1, o2, o3, base):
    level_kernel(SEQ[0], own, g0, g1, g2, base_in, None, base)
    at = lax.axis_index(SEQ[2])
    parts = [p[...].astype(F32) for p in (p0, p1, p2, p3)]
    for mine, out in zip(SLOTS, (o0, o1, o2, o3)):
        run = base[...]
        for step, part in zip(SLOTS, parts):
            run = run + part * ((at ^ step) < (at ^ mine)).astype(F32)
        out[...] = run.astype(BF16)


def small_call(kernel, outs, *args, scratch=()):
    shape = args[0].shape
    return pl.pallas_call(
        kernel,
        out_shape=[jax.ShapeDtypeStruct(shape, kind) for kind in outs],
        in_specs=[VMEM] * len(args),
        out_specs=[VMEM] * len(outs),
        scratch_shapes=list(scratch),
        compiler_params=pltpu.CompilerParams(vmem_limit_bytes=4 * 2**20),
        cost_estimate=pl.CostEstimate(flops=10**6, bytes_accessed=2**20, transcendentals=0),
    )(*args)


def middle_kernel(own, g0, g1, g2, total, base):
    level_kernel(SEQ[1], own, g0, g1, g2, None, total, base)


def exclusive_prefix(states):
    parts = [states[0]] + [partner(state, SEQ[2], step) for step, state in zip(STEPS, states[1:])]
    (low,) = small_call(total_kernel, [BF16], *parts)
    got = [partner(low, SEQ[1], step) for step in STEPS]
    total, base = small_call(middle_kernel, [BF16, F32], low, *got)
    got = [partner(total, SEQ[0], step) for step in STEPS]
    scratch = [pltpu.VMEM(low.shape, F32)]
    outs = small_call(spread_kernel, [BF16] * 4, total, *got, base, *parts, scratch=scratch)
    back = {0: outs[0]}
    for step, out in zip(STEPS, outs[1:]):
        back[step] = partner(out, SEQ[2], step)
    return back


def per_device(tokens, w_query, w_key, w_value, w_out):
    tokens, w_query, w_key, w_value, w_out = (
        pltpu.with_memory_space_constraint(x, pltpu.HBM)
        for x in (tokens, w_query, w_key, w_value, w_out)
    )
    table = jnp.asarray(feature_tables())
    q, kt, val, local, *states, columns = head_stage(
        tokens, w_key, w_query, w_value, w_out
    )
    inner = {}
    args = (q, kt, val, local, table)
    for slot, step in enumerate(SLOTS):
        for h in range(2):
            inner[step, h] = inner_stage(slot, h, *args)
    back = exclusive_prefix(states)

    def outer(steps):
        return outer_stage(
            [back[step] for step in steps],
            [inner[step, h][0] for step in steps for h in range(2)],
            [inner[step, h][1] for step in steps for h in range(2)],
        )

    places, start = ([], 0)
    for steps in GROUPS:
        places.append((start, 256 * len(steps)))
        start += 256 * len(steps)
    own, other = ([], [])
    for steps in GROUPS:
        own.append(outer(steps))
        other.append(lax.ppermute(own[-1], "head", [(0, 1), (1, 0)]))
    mine = [(0, *place) for place in places]
    theirs = [(1, *place) for place in places]
    acc = out_stage(own[:1], mine[:1], columns)
    acc = out_stage([*own[1:], other[0]], (*mine[1:], theirs[0]), columns, acc)
    return out_stage(other[1:], theirs[1:], columns, acc, last=True)


def solution(mesh):
    split = Mesh(
        mesh.devices.reshape(4, 4, 4, mesh.shape["head"]), ("seq_0", "seq_1", "seq_2", "head")
    )
    in_specs = (P(SEQ, None), P(None, "head"), P(None, "head"), P(None, "head"), P())
    out_specs = P(SEQ, "head")
    return jax.shard_map(
        per_device, mesh=split, in_specs=in_specs, out_specs=out_specs, check_vma=False
    )
```
